128 devices in a mesh: rep: 1, ep: 16 (over z, y), fsdp: 8 (over x, core).
Axes of the slice: x: 4, y: 4, z: 4, core: 2. Of those that a mesh axis runs over, the one named last changes fastest.
Arguments:
- x: bfloat16 [32768, 4096], P(('rep', 'ep', 'fsdp'))
- norm_w: float32 [2, 4096], replicated
- router_w: bfloat16 [2, 4096, 16], replicated
- w_gate: bfloat16 [2, 16, 4096, 688], P(None, 'ep', None, 'fsdp')
- w_up: bfloat16 [2, 16, 4096, 688], P(None, 'ep', None, 'fsdp')
- w_down: bfloat16 [2, 16, 688, 4096], P(None, 'ep', 'fsdp')
- expert_idx: int32 [2, 32768, 4], P(None, ('rep', 'ep', 'fsdp'))
Outputs:
- output: bfloat16 [32768, 4096], P(('rep', 'ep', 'fsdp'))
All inputs are finite; a program needn't handle non-finite values.
Results may differ from the reference program's by a relative error of at most 0.0054561.
Values are sent between devices in bfloat16 or wider.
A program may use at most 1 GiB of HBM per device.

```python
import jax
import jax.numpy as jnp
from jax import lax

MODEL_DIM = 4096
FFN_DIM = 688
EXPERTS = 16
TOP_K = 4
LAYERS = 2
TOKENS = 32768
NORM_EPS = 1e-5
ROW_BLOCK = min(TOKENS, 1024)


def draw_routing(key):
    key_noise, key_hot = jax.random.split(key)
    noise_int = jax.random.randint(key_noise, (LAYERS, TOKENS, EXPERTS), 0, 4096)
    hot_bias = jax.random.randint(key_hot, (LAYERS, 1, EXPERTS), 0, 3072)
    expert_ids = jnp.arange(EXPERTS, dtype=jnp.int32)
    cover_bonus = jnp.where((jnp.arange(TOKENS, dtype=jnp.int32) % EXPERTS)[:, None] == expert_ids[None, :], 16384, 0)
    score_int = (noise_int + hot_bias + cover_bonus[None]) * EXPERTS + expert_ids
    return lax.top_k(score_int, TOP_K)[1].astype(jnp.int32)


def setup_inputs(seed: int = 0, part: int = 0) -> dict:
    shared = jax.random.key(seed)
    part_key = jax.random.fold_in(shared, part)
    key_x, key_route = jax.random.split(part_key)
    key_list = jax.random.split(shared, 5)
    x = jax.random.normal(key_x, (TOKENS, MODEL_DIM), jnp.float32).astype(jnp.bfloat16)
    norm_w = 1.0 + 0.5 * jax.random.uniform(key_list[0], (LAYERS, MODEL_DIM), jnp.float32, -1.0, 1.0)
    router_w = (2.0 * MODEL_DIM ** -0.5 * jax.random.normal(key_list[1], (LAYERS, MODEL_DIM, EXPERTS), jnp.float32)).astype(jnp.bfloat16)
    w_gate = (MODEL_DIM ** -0.5 * jax.random.normal(key_list[2], (LAYERS, EXPERTS, MODEL_DIM, FFN_DIM), jnp.float32)).astype(jnp.bfloat16)
    w_up = (MODEL_DIM ** -0.5 * jax.random.normal(key_list[3], (LAYERS, EXPERTS, MODEL_DIM, FFN_DIM), jnp.float32)).astype(jnp.bfloat16)
    w_down = (2.0 * FFN_DIM ** -0.5 * jax.random.normal(key_list[4], (LAYERS, EXPERTS, FFN_DIM, MODEL_DIM), jnp.float32)).astype(jnp.bfloat16)
    expert_idx = draw_routing(key_route)
    return {"x": x, "norm_w": norm_w, "router_w": router_w, "w_gate": w_gate, "w_up": w_up, "w_down": w_down, "expert_idx": expert_idx}


def moe_block(x_blk, idx_blk, norm_w, router_w, w_gate, w_up, w_down):
    x_f32 = x_blk.astype(jnp.float32)
    normed = (x_f32 * lax.rsqrt(jnp.mean(x_f32 * x_f32, axis=-1, keepdims=True) + NORM_EPS) * norm_w).astype(jnp.bfloat16)
    logits = jnp.dot(normed, router_w, preferred_element_type=jnp.float32)
    gate_wts = jax.nn.softmax(jnp.take_along_axis(logits, idx_blk, axis=1), axis=-1)
    expert_ids = jnp.arange(EXPERTS, dtype=jnp.int32)
    coeff_te = jnp.sum(jnp.where(idx_blk[:, :, None] == expert_ids[None, None, :], gate_wts[:, :, None], 0.0), axis=1)

    def expert_step(acc_out, packed):
        gate_e, up_e, down_e, coeff_e = packed
        gate_proj = jnp.dot(normed, gate_e, preferred_element_type=jnp.float32)
        up_proj = jnp.dot(normed, up_e, preferred_element_type=jnp.float32)
        hidden_act = (jax.nn.silu(gate_proj) * up_proj).astype(jnp.bfloat16)
        expert_out = jnp.dot(hidden_act, down_e, preferred_element_type=jnp.float32)
        return acc_out + coeff_e[:, None] * expert_out, None

    init_acc = jnp.zeros((ROW_BLOCK, MODEL_DIM), jnp.float32)
    mixed = lax.scan(expert_step, init_acc, (w_gate, w_up, w_down, coeff_te.T))[0]
    return (x_f32 + mixed).astype(jnp.bfloat16)


def reference(x, norm_w, router_w, w_gate, w_up, w_down, expert_idx):
    blocks = TOKENS // ROW_BLOCK

    def layer_step(x_cur, layer_args):
        norm_l, router_l, gate_l, up_l, down_l, idx_l = layer_args

        def block_fn(packed):
            return moe_block(packed[0], packed[1], norm_l, router_l, gate_l, up_l, down_l)

        new_rows = lax.map(block_fn, (x_cur.reshape(blocks, ROW_BLOCK, MODEL_DIM), idx_l.reshape(blocks, ROW_BLOCK, TOP_K)))
        return new_rows.reshape(TOKENS, MODEL_DIM), None

    return lax.scan(layer_step, x, (norm_w, router_w, w_gate, w_up, w_down, expert_idx))[0]
```

```python
import functools

import jax
import jax.numpy as jnp
from jax import lax
from jax.experimental import pallas as pl
from jax.experimental.pallas import tpu as pltpu
from jax.sharding import PartitionSpec as P

NORM_EPS = 1e-5
TB = 256
D = 4096
FP = 88
E = 16
K = 4
GROUPS = 4
GROWS = E // GROUPS * 2 * FP
BF = jnp.bfloat16
F32 = jnp.float32


def up_kernel(x_ref, nw_ref, idx_ref, w_hbm, rt_hbm, a_ref, g_ref, wv, h, slots, logits, sems):
    step = pl.program_id(0)

    @pl.when(step == 0)
    def _():
        copies = []
        for g in range(GROUPS):
            copies.append(pltpu.make_async_copy(w_hbm.at[pl.ds(g * GROWS, GROWS)], wv.at[g, pl.ds(0, GROWS)], sems.at[2 * g]))
            copies.append(pltpu.make_async_copy(rt_hbm, wv.at[g, pl.ds(GROWS, E)], sems.at[2 * g + 1]))
        for c in copies:
            c.start()
        for c in copies:
            c.wait()

    for tb in range(2):
        def rows(c, tb=tb):
            if x_ref.shape[0] == 2:
                return x_ref[tb, c]
            return x_ref[c, tb]

        def ssq_body(c, acc):
            xf = rows(c).astype(F32)
            return acc + jnp.sum(xf * xf, axis=0, keepdims=True)

        ssq = lax.fori_loop(0, 8, ssq_body, jnp.zeros((1, TB), F32))
        rstd = lax.rsqrt(ssq * (1.0 / D) + NORM_EPS)

        def h_body(c, carry, tb=tb, rstd=rstd):
            xf = rows(c).astype(F32)
            nw = nw_ref[c]
            nw2 = jnp.concatenate([nw, nw], axis=1)
            h[pl.ds(pl.multiple_of(c * 512, 512), 512), tb * TB:(tb + 1) * TB] = (xf * rstd * nw2).astype(BF)
            return carry

        lax.fori_loop(0, 8, h_body, 0)

    slots[...] = jnp.zeros_like(slots)
    idx = jnp.concatenate([idx_ref[0], idx_ref[1]], axis=1)

    def group(g, carry):
        res = jnp.dot(wv[g], h[...], preferred_element_type=F32)
        logits[...] = res[GROWS:]
        for k in range(E // GROUPS):
            u = res[k * 2 * FP:k * 2 * FP + FP]
            v = res[k * 2 * FP + FP:(k + 1) * 2 * FP]
            act = jax.nn.silu(u) * v
            e = g * (E // GROUPS) + k
            for j in range(K):
                slots[j] = jnp.where(idx[j:j + 1] == e, act, slots[j])
        return carry

    lax.fori_loop(0, GROUPS, group, 0)
    for tb in range(2):
        a_ref[tb] = slots[:, :, tb * TB:(tb + 1) * TB].astype(BF)
    eids = lax.broadcasted_iota(jnp.int32, (E, 2 * TB), 0)
    chosen = idx[0:1] == eids
    for j in range(1, K):
        chosen = jnp.logical_or(chosen, idx[j:j + 1] == eids)
    lg = jnp.where(chosen, logits[...], -jnp.inf)
    ex = jnp.where(chosen, jnp.exp(lg - jnp.max(lg, axis=0, keepdims=True)), 0.0)
    gates = ex / jnp.sum(ex, axis=0, keepdims=True)
    for tb in range(2):
        g_ref[tb] = gates[:, tb * TB:(tb + 1) * TB]


def up_proj(x, nw, idx, w, rt, tok_major):
    if tok_major:
        x_spec = pl.BlockSpec((2, 8, 512, TB), lambda i: (i, 0, 0, 0))
    else:
        x_spec = pl.BlockSpec((8, 2, 512, TB), lambda i: (0, i, 0, 0))
    return pl.pallas_call(
        up_kernel,
        grid=(4,),
        out_shape=(jax.ShapeDtypeStruct((8, K, FP, TB), BF), jax.ShapeDtypeStruct((8, E, TB), F32)),
        in_specs=[
            x_spec,
            pl.BlockSpec((8, 512, 128), lambda i: (0, 0, 0)),
            pl.BlockSpec((2, K, TB), lambda i: (i, 0, 0)),
            pl.BlockSpec(memory_space=pl.ANY),
            pl.BlockSpec(memory_space=pl.ANY),
        ],
        out_specs=(pl.BlockSpec((2, K, FP, TB), lambda i: (i, 0, 0, 0)), pl.BlockSpec((2, E, TB), lambda i: (i, 0, 0))),
        scratch_shapes=[
            pltpu.VMEM((GROUPS, GROWS + E, D), BF),
            pltpu.VMEM((D, 2 * TB), BF),
            pltpu.VMEM((K, FP, 2 * TB), F32),
            pltpu.VMEM((E, 2 * TB), F32),
            pltpu.SemaphoreType.DMA((2 * GROUPS,)),
        ],
        compiler_params=pltpu.CompilerParams(vmem_limit_bytes=60 * 1024 * 1024),
        cost_estimate=pl.CostEstimate(flops=2 * 2832 * D * 2048, bytes_accessed=45_000_000, transcendentals=3_000_000),
        name="up_proj",
    )(x, nw, idx, w, rt)


def down_kernel(a_ref, idx_ref, g_ref, x_ref, wd_ref, o_ref, acc):
    idx = jnp.concatenate([idx_ref[0], idx_ref[1]], axis=1).astype(F32).astype(BF)
    gates = jnp.concatenate([g_ref[0], g_ref[1]], axis=1)
    acc[...] = jnp.zeros_like(acc)
    for e in range(E):
        parts = []
        for tb in range(2):
            sel = jnp.zeros((8 * FP, TB), BF)
            for j in range(K):
                row = idx[j:j + 1, tb * TB:(tb + 1) * TB]
                sel = jnp.where(row == jnp.asarray(e, BF), a_ref[tb, j], sel)
            parts.append(sel)
        out = jnp.dot(wd_ref[e], jnp.concatenate(parts, axis=1), preferred_element_type=F32)
        acc[...] += gates[e:e + 1] * out
    for tb in range(2):
        o_ref[tb] = (x_ref[tb].astype(F32) + acc[:, tb * TB:(tb + 1) * TB]).astype(BF)


def down_proj(a, idx, gates, xs, wd):
    return pl.pallas_call(
        down_kernel,
        grid=(4,),
        out_shape=jax.ShapeDtypeStruct((8, 512, TB), BF),
        in_specs=[
            pl.BlockSpec((2, K, 8 * FP, TB), lambda i: (i, 0, 0, 0)),
            pl.BlockSpec((2, K, TB), lambda i: (i, 0, 0)),
            pl.BlockSpec((2, E, TB), lambda i: (i, 0, 0)),
            pl.BlockSpec((2, 512, TB), lambda i: (i, 0, 0)),
            pl.BlockSpec((E, 512, 8 * FP), lambda i: (0, 0, 0)),
        ],
        out_specs=pl.BlockSpec((2, 512, TB), lambda i: (i, 0, 0)),
        scratch_shapes=[pltpu.VMEM((512, 2 * TB), F32)],
        compiler_params=pltpu.CompilerParams(vmem_limit_bytes=60 * 1024 * 1024),
        cost_estimate=pl.CostEstimate(flops=2 * 704 * 16 * 512 * 2048, bytes_accessed=30_000_000, transcendentals=0),
        name="down_proj",
    )(a, idx, gates, xs, wd)


def solution(mesh):
    tok_spec = P(("rep", "ep", "fsdp"), None)
    idx_spec = P(None, ("rep", "ep", "fsdp"), None)
    in_specs = (tok_spec, P(None, None), P(None, None, None), P(None, "ep", None, "fsdp"), P(None, "ep", None, "fsdp"), P(None, "ep", "fsdp", None), idx_spec)

    def local_program(x, norm_w, router_w, w_gate, w_up, w_down, expert_idx):
        layers = norm_w.shape[0]
        me = lax.axis_index("fsdp")
        ups = []
        for l in range(layers):
            pad = jnp.zeros((FP - 86, D), BF)
            rows = jnp.concatenate([w_gate[l, 0].T, pad, w_up[l, 0].T, pad], axis=0)
            ups.append(lax.all_gather(rows, "ep", axis=0, tiled=True))
        wd = jnp.pad(w_down[:, 0], ((0, 0), (0, FP - 86), (0, 0)))
        wd = lax.all_to_all(wd, "fsdp", split_axis=2, concat_axis=1, tiled=True)
        wd = jnp.swapaxes(wd, 1, 2)
        downs = [lax.all_gather(wd[l], "ep", axis=0, tiled=False) for l in range(layers)]
        xt = x.T.reshape(8, 512, TB)
        xs_all = lax.all_gather(xt, "fsdp", axis=0, tiled=False)
        idx_all = lax.all_gather(jnp.swapaxes(expert_idx, 1, 2), "fsdp", axis=0, tiled=False)
        xs = lax.dynamic_index_in_dim(xs_all, me, axis=1, keepdims=False)
        for l in range(layers):
            nw = jnp.broadcast_to(norm_w[l].reshape(8, 512, 1), (8, 512, 128))
            a, gates = up_proj(xs_all, nw, idx_all[:, l], ups[l], router_w[l].T, l == 0)
            a_all = lax.all_gather(a, "fsdp", axis=2, tiled=True)
            xs = down_proj(a_all, idx_all[:, l], gates, xs, downs[l])
            if l + 1 < layers:
                xs_all = lax.all_gather(xs, "fsdp", axis=0, tiled=False)
        y = lax.all_to_all(xs, "fsdp", split_axis=0, concat_axis=0, tiled=True)
        return y.reshape(D, TB).T

    return jax.shard_map(local_program, mesh=mesh, in_specs=in_specs, out_specs=tok_spec, check_vma=False)
```

```python
import functools

import jax
import jax.numpy as jnp
from jax import lax
from jax.experimental import pallas as pl
from jax.experimental.pallas import tpu as pltpu
from jax.sharding import PartitionSpec as P

NORM_EPS = 1e-5
TB = 256
D = 4096
FP = 88
KP = 768
E = 16
K = 4
GROUPS = 4
GROWS = E // GROUPS * 2 * FP
BF = jnp.bfloat16
F32 = jnp.float32


def up_kernel(x_ref, nw_ref, idx_ref, w_hbm, rt_hbm, a_ref, g_ref, wv, h, slots, logits, sems):
    step = pl.program_id(0)

    @pl.when(step == 0)
    def _():
        copies = []
        for g in range(GROUPS):
            copies.append(pltpu.make_async_copy(w_hbm.at[pl.ds(g * GROWS, GROWS)], wv.at[g, pl.ds(0, GROWS)], sems.at[2 * g]))
            copies.append(pltpu.make_async_copy(rt_hbm, wv.at[g, pl.ds(GROWS, E)], sems.at[2 * g + 1]))
        for c in copies:
            c.start()

    for tb in range(2):
        def rows(c, tb=tb):
            if x_ref.shape[0] == 2:
                return x_ref[tb, c]
            return x_ref[c, tb]

        def ssq_body(c, acc):
            xf = rows(c).astype(F32)
            return acc + jnp.sum(xf * xf, axis=0, keepdims=True)

        ssq = lax.fori_loop(0, 8, ssq_body, jnp.zeros((1, TB), F32))
        rstd = lax.rsqrt(ssq * (1.0 / D) + NORM_EPS)

        def h_body(c, carry, tb=tb, rstd=rstd):
            xf = rows(c).astype(F32)
            nw = nw_ref[c]
            nw2 = jnp.concatenate([nw, nw], axis=1)
            h[pl.ds(pl.multiple_of(c * 512, 512), 512), tb * TB:(tb + 1) * TB] = (xf * rstd * nw2).astype(BF)
            return carry

        lax.fori_loop(0, 8, h_body, 0)

    slots[...] = jnp.zeros_like(slots)
    idx = jnp.concatenate([idx_ref[0], idx_ref[1]], axis=1)

    def group(g, carry):
        @pl.when(step == 0)
        def _():
            pltpu.make_async_copy(w_hbm.at[pl.ds(g * GROWS, GROWS)], wv.at[g, pl.ds(0, GROWS)], sems.at[2 * g]).wait()
            pltpu.make_async_copy(rt_hbm, wv.at[g, pl.ds(GROWS, E)], sems.at[2 * g + 1]).wait()

        res = jnp.dot(wv[g], h[...], preferred_element_type=F32)
        logits[...] = res[GROWS:]
        for k in range(E // GROUPS):
            u = res[k * 2 * FP:k * 2 * FP + FP]
            v = res[k * 2 * FP + FP:(k + 1) * 2 * FP]
            act = jax.nn.silu(u) * v
            e = g * (E // GROUPS) + k
            for j in range(K):
                slots[j] = jnp.where(idx[j:j + 1] == e, act, slots[j])
        return carry

    lax.fori_loop(0, GROUPS, group, 0)
    for tb in range(2):
        a_ref[tb] = slots[:, :, tb * TB:(tb + 1) * TB].astype(BF)
    eids = lax.broadcasted_iota(jnp.int32, (E, 2 * TB), 0)
    chosen = idx[0:1] == eids
    for j in range(1, K):
        chosen = jnp.logical_or(chosen, idx[j:j + 1] == eids)
    lg = jnp.where(chosen, logits[...], -jnp.inf)
    ex = jnp.where(chosen, jnp.exp(lg - jnp.max(lg, axis=0, keepdims=True)), 0.0)
    gates = ex / jnp.sum(ex, axis=0, keepdims=True)
    for tb in range(2):
        g_ref[tb] = gates[:, tb * TB:(tb + 1) * TB]


def up_proj(x, nw, idx, w, rt, tok_major):
    if tok_major:
        x_spec = pl.BlockSpec((2, 8, 512, TB), lambda i: (i, 0, 0, 0))
    else:
        x_spec = pl.BlockSpec((8, 2, 512, TB), lambda i: (0, i, 0, 0))
    return pl.pallas_call(
        up_kernel,
        grid=(4,),
        out_shape=(jax.ShapeDtypeStruct((8, K, FP, TB), BF), jax.ShapeDtypeStruct((8, E, TB), F32)),
        in_specs=[
            x_spec,
            pl.BlockSpec((8, 512, 128), lambda i: (0, 0, 0)),
            pl.BlockSpec((2, K, TB), lambda i: (i, 0, 0)),
            pl.BlockSpec(memory_space=pl.ANY),
            pl.BlockSpec(memory_space=pl.ANY),
        ],
        out_specs=(pl.BlockSpec((2, K, FP, TB), lambda i: (i, 0, 0, 0)), pl.BlockSpec((2, E, TB), lambda i: (i, 0, 0))),
        scratch_shapes=[
            pltpu.VMEM((GROUPS, GROWS + E, D), BF),
            pltpu.VMEM((D, 2 * TB), BF),
            pltpu.VMEM((K, FP, 2 * TB), F32),
            pltpu.VMEM((E, 2 * TB), F32),
            pltpu.SemaphoreType.DMA((2 * GROUPS,)),
        ],
        compiler_params=pltpu.CompilerParams(vmem_limit_bytes=60 * 1024 * 1024),
        cost_estimate=pl.CostEstimate(flops=2 * 2832 * D * 2048, bytes_accessed=45_000_000, transcendentals=3_000_000),
        name="up_proj",
    )(x, nw, idx, w, rt)


def down_kernel(a_ref, idx_ref, g_ref, x_ref, wd_ref, o_ref, acc):
    idx = jnp.concatenate([idx_ref[0], idx_ref[1]], axis=1).astype(F32).astype(BF)
    acc[...] = jnp.zeros_like(acc)

    def group(g, carry):
        for k in range(E // GROUPS):
            e = g * (E // GROUPS) + k
            ef = e.astype(F32).astype(BF)
            parts = []
            for tb in range(2):
                sel = jnp.zeros((8 * FP, TB), BF)
                for j in range(K):
                    row = idx[j:j + 1, tb * TB:(tb + 1) * TB]
                    sel = jnp.where(row == ef, a_ref[tb, j], sel)
                parts.append(sel)
            out = jnp.dot(wd_ref[e, :, :8 * FP], jnp.concatenate(parts, axis=1), preferred_element_type=F32)
            gate = jnp.concatenate([g_ref[0, pl.ds(e, 1)], g_ref[1, pl.ds(e, 1)]], axis=1)
            acc[...] += gate * out
        return carry

    lax.fori_loop(0, GROUPS, group, 0)
    for tb in range(2):
        o_ref[tb] = (x_ref[tb].astype(F32) + acc[:, tb * TB:(tb + 1) * TB]).astype(BF)


def down_proj(a, idx, gates, xs, wd):
    return pl.pallas_call(
        down_kernel,
        grid=(4,),
        out_shape=jax.ShapeDtypeStruct((8, 512, TB), BF),
        in_specs=[
            pl.BlockSpec((2, K, 8 * FP, TB), lambda i: (i, 0, 0, 0)),
            pl.BlockSpec((2, K, TB), lambda i: (i, 0, 0)),
            pl.BlockSpec((2, E, TB), lambda i: (i, 0, 0)),
            pl.BlockSpec((2, 512, TB), lambda i: (i, 0, 0)),
            pl.BlockSpec((E, 512, KP), lambda i: (0, 0, 0)),
        ],
        out_specs=pl.BlockSpec((2, 512, TB), lambda i: (i, 0, 0)),
        scratch_shapes=[pltpu.VMEM((512, 2 * TB), F32)],
        compiler_params=pltpu.CompilerParams(vmem_limit_bytes=60 * 1024 * 1024),
        cost_estimate=pl.CostEstimate(flops=2 * 704 * 16 * 512 * 2048, bytes_accessed=30_000_000, transcendentals=0),
        name="down_proj",
    )(a, idx, gates, xs, wd)


MESH = pl.DeviceIdType.MESH
CH = 4


def ring_position():
    f = lax.axis_index("fsdp")
    ring, core = f // 2, f % 2

    def at(step, other=0):
        c = core if other == 0 else 1 - core
        return lax.rem(ring + step, 4) * 2 + c

    return f, at


def greet(peers):
    barrier = pltpu.get_barrier_semaphore()
    for p in peers:
        pl.semaphore_signal(barrier, inc=1, device_id={"fsdp": p}, device_id_type=MESH)
    pl.semaphore_wait(barrier, len(peers))


def ring_gather(own, place, send_sem, recv_sem):
    f, at = ring_position()
    left, right, partner = at(3), at(1), at(0, 1)

    def copy(kind, k, src, owner, target):
        return pltpu.make_async_remote_copy(
            src_ref=src, dst_ref=place(owner, k), send_sem=send_sem.at[kind, k], recv_sem=recv_sem.at[kind, k],
            device_id={"fsdp": target}, device_id_type=MESH)

    sent = []

    def send(kind, k, src, owner, target):
        c = copy(kind, k, src, owner, target)
        c.start()
        sent.append(c)

    def arrived(kind, k, owner):
        copy(kind, k, place(owner, k), owner, left).wait_recv()

    def start():
        for k in range(CH):
            send(0, k, own(k), f, right)
            send(1, k, own(k), f, left)
            send(2, k, own(k), f, partner)

    def finish():
        for k in range(CH):
            arrived(0, k, at(3))
            if k < CH // 2:
                send(3, k, place(at(3), k), at(3), right)
            send(4, k, place(at(3), k), at(3), partner)
            arrived(1, k, at(1))
            if k >= CH // 2:
                send(3, k, place(at(1), k), at(1), left)
            send(5, k, place(at(1), k), at(1), partner)
        for i in range(CH // 2):
            for k in (i, i + CH // 2):
                arrived(3, k, at(2))
                send(6, k, place(at(2), k), at(2), partner)
        for kind, owner in ((2, at(0, 1)), (4, at(3, 1)), (5, at(1, 1)), (6, at(2, 1))):
            for k in range(CH):
                arrived(kind, k, owner)
        for c in sent:
            c.wait_send()

    return start, finish


RING_SEMS = [pltpu.SemaphoreType.DMA((7, CH)), pltpu.SemaphoreType.DMA((7, CH))]


def others(at):
    return [at(s, o) for s in range(4) for o in range(2) if (s, o) != (0, 0)]


def first_kernel(x_ref, idx_ref, wd_ref, x_all, idx_all, wd_all, send_sem, recv_sem, local_sem, psend, precv):
    f, at = ring_position()
    peers = [(s, o) for s in range(4) for o in range(2) if (s, o) != (0, 0)]
    greet(others(at))
    n = 8 // CH
    start, finish = ring_gather(lambda k: x_ref.at[pl.ds(k * n, n)], lambda owner, k: x_all.at[owner, pl.ds(k * n, n)], send_sem, recv_sem)
    locals_ = [
        pltpu.make_async_copy(x_ref, x_all.at[f], local_sem.at[0]),
        pltpu.make_async_copy(idx_ref, idx_all.at[f], local_sem.at[1]),
        pltpu.make_async_copy(wd_ref.at[:, f], wd_all.at[:, f], local_sem.at[2]),
    ]
    for c in locals_:
        c.start()
    small = []
    for p, (s, o) in enumerate(peers):
        small.append(pltpu.make_async_remote_copy(
            src_ref=idx_ref, dst_ref=idx_all.at[f], send_sem=psend.at[0, p], recv_sem=precv.at[0, p],
            device_id={"fsdp": at(s, o)}, device_id_type=MESH))
        small.append(pltpu.make_async_remote_copy(
            src_ref=wd_ref.at[:, at(s, o)], dst_ref=wd_all.at[:, f], send_sem=psend.at[1, p], recv_sem=precv.at[1, p],
            device_id={"fsdp": at(s, o)}, device_id_type=MESH))
    for c in small:
        c.start()
    start()
    finish()
    for p, (s, o) in enumerate(peers):
        source = at((4 - s) % 4, o)
        for kind, (src, dst) in enumerate(((idx_ref, idx_all.at[source]), (wd_ref.at[:, 0], wd_all.at[:, source]))):
            pltpu.make_async_remote_copy(
                src_ref=src, dst_ref=dst, send_sem=psend.at[kind, p], recv_sem=precv.at[kind, p],
                device_id={"fsdp": source}, device_id_type=MESH).wait_recv()
    for c in small:
        c.wait_send()
    for c in locals_:
        c.wait()


def first_exchange(xt, idx, wd):
    return pl.pallas_call(
        first_kernel,
        out_shape=(jax.ShapeDtypeStruct((8, 8, 512, TB), BF), jax.ShapeDtypeStruct((8, 2, K, TB), jnp.int32), jax.ShapeDtypeStruct((2, 8, FP, 512), BF)),
        in_specs=[pl.BlockSpec(memory_space=pltpu.VMEM)] * 3,
        out_specs=[pl.BlockSpec(memory_space=pl.ANY)] * 3,
        scratch_shapes=RING_SEMS + [pltpu.SemaphoreType.DMA((3,)), pltpu.SemaphoreType.DMA((2, 7)), pltpu.SemaphoreType.DMA((2, 7))],
        compiler_params=pltpu.CompilerParams(collective_id=0, has_side_effects=True),
        cost_estimate=pl.CostEstimate(flops=70_000_000_000, bytes_accessed=16_000_000, transcendentals=0),
        name="first_exchange",
    )(xt, idx, wd)


def x_gather_kernel(x_ref, x_all, send_sem, recv_sem, local_sem):
    f, at = ring_position()
    greet([at(3), at(1), at(0, 1)])
    n = 8 // CH
    start, finish = ring_gather(lambda k: x_ref.at[pl.ds(k * n, n)], lambda owner, k: x_all.at[owner, pl.ds(k * n, n)], send_sem, recv_sem)
    mine = pltpu.make_async_copy(x_ref, x_all.at[f], local_sem)
    mine.start()
    start()
    finish()
    mine.wait()


def x_gather(xs):
    return pl.pallas_call(
        x_gather_kernel,
        out_shape=jax.ShapeDtypeStruct((8, 8, 512, TB), BF),
        in_specs=[pl.BlockSpec(memory_space=pltpu.VMEM)],
        out_specs=pl.BlockSpec(memory_space=pl.ANY),
        scratch_shapes=RING_SEMS + [pltpu.SemaphoreType.DMA],
        compiler_params=pltpu.CompilerParams(collective_id=1, has_side_effects=True),
        cost_estimate=pl.CostEstimate(flops=70_000_000_000, bytes_accessed=16_000_000, transcendentals=0),
        name="x_gather",
    )(xs)


def a_gather_kernel(a_ref, a_all, send_sem, recv_sem, local_sem):
    f, at = ring_position()
    greet([at(3), at(1), at(0, 1)])
    n = 8 // CH

    def place(owner, k):
        return a_all.at[pl.ds(k * n, n), :, pl.ds(pl.multiple_of(owner * FP, 8), FP)]

    start, finish = ring_gather(lambda k: a_ref.at[pl.ds(k * n, n)], place, send_sem, recv_sem)
    mine = pltpu.make_async_copy(a_ref, a_all.at[:, :, pl.ds(pl.multiple_of(f * FP, 8), FP)], local_sem)
    mine.start()
    start()
    finish()
    mine.wait()


def a_gather(a):
    return pl.pallas_call(
        a_gather_kernel,
        out_shape=jax.ShapeDtypeStruct((8, K, 8 * FP, TB), BF),
        in_specs=[pl.BlockSpec(memory_space=pltpu.VMEM)],
        out_specs=pl.BlockSpec(memory_space=pl.ANY),
        scratch_shapes=RING_SEMS + [pltpu.SemaphoreType.DMA],
        compiler_params=pltpu.CompilerParams(collective_id=2, has_side_effects=True),
        cost_estimate=pl.CostEstimate(flops=50_000_000_000, bytes_accessed=12_000_000, transcendentals=0),
        name="a_gather",
    )(a)


def last_kernel(y_ref, o_ref, local_sem, psend, precv):
    f, at = ring_position()
    peers = [(s, o) for s in range(4) for o in range(2) if (s, o) != (0, 0)]
    greet(others(at))
    mine = pltpu.make_async_copy(y_ref.at[f], o_ref.at[f], local_sem)
    mine.start()
    copies = []
    for p, (s, o) in enumerate(peers):
        c = pltpu.make_async_remote_copy(
            src_ref=y_ref.at[at(s, o)], dst_ref=o_ref.at[f], send_sem=psend.at[p], recv_sem=precv.at[p],
            device_id={"fsdp": at(s, o)}, device_id_type=MESH)
        c.start()
        copies.append(c)
    for p, (s, o) in enumerate(peers):
        source = at((4 - s) % 4, o)
        pltpu.make_async_remote_copy(
            src_ref=y_ref.at[0], dst_ref=o_ref.at[source], send_sem=psend.at[p], recv_sem=precv.at[p],
            device_id={"fsdp": source}, device_id_type=MESH).wait_recv()
    for c in copies:
        c.wait_send()
    mine.wait()


def last_exchange(y):
    return pl.pallas_call(
        last_kernel,
        out_shape=jax.ShapeDtypeStruct((8, 512, TB), BF),
        in_specs=[pl.BlockSpec(memory_space=pltpu.VMEM)],
        out_specs=pl.BlockSpec(memory_space=pl.ANY),
        scratch_shapes=[pltpu.SemaphoreType.DMA, pltpu.SemaphoreType.DMA((7,)), pltpu.SemaphoreType.DMA((7,))],
        compiler_params=pltpu.CompilerParams(collective_id=3, has_side_effects=True),
        cost_estimate=pl.CostEstimate(flops=20_000_000_000, bytes_accessed=4_000_000, transcendentals=0),
        name="last_exchange",
    )(y)


def solution(mesh):
    tok_spec = P(("rep", "ep", "fsdp"), None)
    idx_spec = P(None, ("rep", "ep", "fsdp"), None)
    in_specs = (tok_spec, P(None, None), P(None, None, None), P(None, "ep", None, "fsdp"), P(None, "ep", None, "fsdp"), P(None, "ep", "fsdp", None), idx_spec)

    def local_program(x, norm_w, router_w, w_gate, w_up, w_down, expert_idx):
        layers = norm_w.shape[0]
        me = lax.axis_index("fsdp")
        pad = jnp.zeros((FP - 86, D), BF)
        rows = [jnp.concatenate([w_gate[l, 0].T, pad, w_up[l, 0].T, pad], axis=0) for l in range(layers)]
        ups = [lax.all_gather(rows[0], "ep", axis=0, tiled=True)]
        xt = x.T.reshape(8, 512, TB)
        wd = jnp.pad(w_down[:, 0], ((0, 0), (0, FP - 86), (0, 0))).reshape(layers, FP, 8, 512).swapaxes(1, 2)
        xt, idx, wd, _ = lax.optimization_barrier((xt, jnp.swapaxes(expert_idx, 1, 2), wd, rows[0]))
        xs_all, idx_all, wd = first_exchange(xt, idx, wd)

        def gather_down(block):
            block = jnp.swapaxes(block.reshape(8 * FP, 512), 0, 1)
            return lax.all_gather(jnp.pad(block, ((0, 0), (0, KP - 8 * FP))), "ep", axis=0, tiled=False)

        downs = [gather_down(wd[0])]
        xs = lax.dynamic_index_in_dim(xs_all, me, axis=1, keepdims=False)
        for l in range(layers):
            nw = jnp.broadcast_to(norm_w[l].reshape(8, 512, 1), (8, 512, 128))
            a, gates = up_proj(xs_all, nw, idx_all[:, l], ups[l], router_w[l].T, l == 0)
            if l + 1 < layers:
                nxt, _ = lax.optimization_barrier((rows[l + 1], a))
                ups.append(lax.all_gather(nxt, "ep", axis=0, tiled=True))
            xs = down_proj(a_gather(a), idx_all[:, l], gates, xs, downs[l])
            if l + 1 < layers:
                nxt, _ = lax.optimization_barrier((wd[l + 1], xs))
                downs.append(gather_down(nxt))
                xs_all = x_gather(xs)
        return last_exchange(xs).reshape(D, TB).T

    return jax.shard_map(local_program, mesh=mesh, in_specs=in_specs, out_specs=tok_spec, check_vma=False)
```

```python
import functools

import jax
import jax.numpy as jnp
from jax import lax
from jax.experimental import pallas as pl
from jax.experimental.pallas import tpu as pltpu
from jax.sharding import PartitionSpec as P

NORM_EPS = 1e-5
TB = 256
D = 4096
FP = 88
KP = 768
E = 16
K = 4
GROUPS = 4
GROWS = E // GROUPS * 2 * FP
HALF = 256
BF = jnp.bfloat16
F32 = jnp.float32
MESH = pl.DeviceIdType.MESH
PEERS = [(s, o) for s in range(4) for o in range(2) if (s, o) != (0, 0)]


def fsdp_at(step, other=0):
    f = lax.axis_index("fsdp")
    core = f % 2
    return lax.rem(f // 2 + step, 4) * 2 + (1 - core if other else core)


def greet(devices):
    barrier = pltpu.get_barrier_semaphore()
    for d in devices:
        pl.semaphore_signal(barrier, inc=1, device_id=d, device_id_type=MESH)
    pl.semaphore_wait(barrier, len(devices))


class Ring:
    def __init__(self, pos, dev, own, place, chunks, send_sem, recv_sem, partner=None):
        self.pos, self.dev, self.own, self.place, self.chunks = pos, dev, own, place, chunks
        self.send_sem, self.recv_sem, self.partner = send_sem, recv_sem, partner

    def at(self, step):
        return lax.rem(self.pos + step, 4)

    def copy(self, kind, k, src, dst, device):
        return pltpu.make_async_remote_copy(
            src_ref=src, dst_ref=dst, send_sem=self.send_sem.at[kind, k], recv_sem=self.recv_sem.at[kind, k],
            device_id=device, device_id_type=MESH)

    def own_copies(self, k):
        mine = self.place(self.pos, k)
        out = [self.copy(0, k, self.own(k), mine, self.dev(self.at(1))), self.copy(1, k, self.own(k), mine, self.dev(self.at(3)))]
        if self.partner is not None:
            out.append(self.copy(3, k, self.own(k), mine, self.partner))
        return out

    def onward(self, k, odd):
        source, target = (self.at(1), self.at(3)) if odd else (self.at(3), self.at(1))
        ref = self.place(source, k)
        return self.copy(2, k, ref, ref, self.dev(target))

    def across(self, kind, k):
        ref = self.place(self.at({4: 3, 5: 1, 6: 2}[kind]), k)
        return self.copy(kind, k, ref, ref, self.partner)

    def arrived(self, kind, k, step, other=0):
        ref = self.place(self.at(step), k, 1) if other else self.place(self.at(step), k)
        self.copy(kind, k, ref, ref, self.dev(self.at(1))).wait_recv()

    def start(self, k):
        for c in self.own_copies(k):
            c.start()

    def relay(self, k, odd):
        self.arrived(0, k, 3)
        if not odd:
            self.onward(k, odd).start()
        if self.partner is not None:
            self.across(4, k).start()
        self.arrived(1, k, 1)
        if odd:
            self.onward(k, odd).start()
        if self.partner is not None:
            self.across(5, k).start()

    def last(self, k):
        self.arrived(2, k, 2)
        if self.partner is not None:
            self.across(6, k).start()

    def drain(self):
        for k in range(self.chunks):
            if self.partner is not None:
                for kind, step in ((3, 0), (4, 3), (5, 1), (6, 2)):
                    self.arrived(kind, k, step, 1)
            for c in self.own_copies(k):
                c.wait_send()
            self.onward(k, k % 2 == 1).wait_send()
            if self.partner is not None:
                for kind in (4, 5, 6):
                    self.across(kind, k).wait_send()


def x_ring(own, place, send_sem, recv_sem):
    f = lax.axis_index("fsdp")
    core = f % 2

    def where(p, k, other=0):
        return place(p * 2 + (1 - core if other else core), k)

    return Ring(f // 2, lambda p: {"fsdp": p * 2 + core}, own, where, 8, send_sem, recv_sem, {"fsdp": fsdp_at(0, 1)})


X_SEMS = [pltpu.SemaphoreType.DMA((7, 8)), pltpu.SemaphoreType.DMA((7, 8))]


def x_neighbours():
    return [{"fsdp": fsdp_at(1)}, {"fsdp": fsdp_at(3)}, {"fsdp": fsdp_at(0, 1)}]


def first_kernel(x_ref, idx_ref, wd_ref, x_all, idx_all, wd_all, send_sem, recv_sem, local_sem, psend, precv):
    f = lax.axis_index("fsdp")
    greet([{"fsdp": fsdp_at(s, o)} for s, o in PEERS])
    ring = x_ring(lambda k: x_ref.at[k], lambda owner, k: x_all.at[owner, k], send_sem, recv_sem)
    locals_ = [
        pltpu.make_async_copy(x_ref, x_all.at[f], local_sem.at[0]),
        pltpu.make_async_copy(idx_ref, idx_all.at[f], local_sem.at[1]),
        pltpu.make_async_copy(wd_ref.at[:, f], wd_all.at[:, f], local_sem.at[2]),
    ]
    for c in locals_:
        c.start()
    small = []
    for p, (s, o) in enumerate(PEERS):
        peer = fsdp_at(s, o)
        small.append(pltpu.make_async_remote_copy(
            src_ref=idx_ref, dst_ref=idx_all.at[f], send_sem=psend.at[0, p], recv_sem=precv.at[0, p],
            device_id={"fsdp": peer}, device_id_type=MESH))
        small.append(pltpu.make_async_remote_copy(
            src_ref=wd_ref.at[:, peer], dst_ref=wd_all.at[:, f], send_sem=psend.at[1, p], recv_sem=precv.at[1, p],
            device_id={"fsdp": peer}, device_id_type=MESH))
    for c in small:
        c.start()
    for k in range(8):
        ring.start(k)
    for k in range(8):
        ring.relay(k, k % 2 == 1)
    for k in range(8):
        ring.last(k)
    ring.drain()
    for p, (s, o) in enumerate(PEERS):
        source = fsdp_at((4 - s) % 4, o)
        for kind, (src, dst) in enumerate(((idx_ref, idx_all.at[source]), (wd_ref.at[:, 0], wd_all.at[:, source]))):
            pltpu.make_async_remote_copy(
                src_ref=src, dst_ref=dst, send_sem=psend.at[kind, p], recv_sem=precv.at[kind, p],
                device_id={"fsdp": source}, device_id_type=MESH).wait_recv()
    for c in small:
        c.wait_send()
    for c in locals_:
        c.wait()


def first_exchange(xt, idx, wd):
    return pl.pallas_call(
        first_kernel,
        out_shape=(jax.ShapeDtypeStruct((8, 8, 512, TB), BF), jax.ShapeDtypeStruct((8, 2, K, TB), jnp.int32), jax.ShapeDtypeStruct((2, 8, FP, 512), BF)),
        in_specs=[pl.BlockSpec(memory_space=pltpu.VMEM)] * 3,
        out_specs=[pl.BlockSpec(memory_space=pl.ANY)] * 3,
        scratch_shapes=X_SEMS + [pltpu.SemaphoreType.DMA((3,)), pltpu.SemaphoreType.DMA((2, 7)), pltpu.SemaphoreType.DMA((2, 7))],
        compiler_params=pltpu.CompilerParams(collective_id=0, has_side_effects=True),
        cost_estimate=pl.CostEstimate(flops=70_000_000_000, bytes_accessed=16_000_000, transcendentals=0),
        name="first_exchange",
    )(xt, idx, wd)


def wd_rings(wd_ref, wd_all, send1, recv1, send2, recv2):
    e = lax.axis_index("ep")
    z, y = e // 4, e % 4
    on_y = lambda p: {"ep": z * 4 + p}
    on_z = lambda p: {"ep": p * 4 + y}
    rows = lambda b, k: pl.ds(b * HALF + k * (HALF // 2), HALF // 2)
    first = [
        Ring(y, on_y, lambda k: wd_ref.at[rows(0, k)], lambda p, k: wd_all.at[z * 4 + p, rows(0, k)], 2, send1.at[0], recv1.at[0]),
        Ring(z, on_z, lambda k: wd_ref.at[rows(1, k)], lambda p, k: wd_all.at[p * 4 + y, rows(1, k)], 2, send1.at[1], recv1.at[1]),
    ]
    by_z = lambda p, k: wd_all.at[p * 4 + k, pl.ds(0, HALF)]
    by_y = lambda p, k: wd_all.at[k * 4 + p, pl.ds(HALF, HALF)]
    second = [
        Ring(z, on_z, lambda k: by_z(z, k), by_z, 4, send2.at[0], recv2.at[0]),
        Ring(y, on_y, lambda k: by_y(y, k), by_y, 4, send2.at[1], recv2.at[1]),
    ]
    near = [on_y(lax.rem(y + 1, 4)), on_y(lax.rem(y + 3, 4)), on_z(lax.rem(z + 1, 4)), on_z(lax.rem(z + 3, 4))]
    return first, second, near


def up_kernel(
    x_ref, nw_ref, idx_ref, wd_ref, w_hbm, rt_hbm, a_all, g_ref, wd_all,
    wv, h, slots, logits, a_buf, sems, send_sem, recv_sem, send1, recv1, send2, recv2, local_sem,
):
    step = pl.program_id(0)
    f = lax.axis_index("fsdp")
    mine = lambda owner: pl.ds(pl.multiple_of(owner * FP, 8), FP)
    ring = x_ring(lambda k: a_buf.at[k], lambda owner, k: a_all.at[k, :, mine(owner)], send_sem, recv_sem)
    first, second, near = wd_rings(wd_ref, wd_all, send1, recv1, send2, recv2)
    own_wd = pltpu.make_async_copy(wd_ref, wd_all.at[lax.axis_index("ep")], local_sem.at[8])

    def own_a(k):
        return pltpu.make_async_copy(a_buf.at[k], a_all.at[k, :, mine(f)], local_sem.at[k])

    @pl.when(step == 0)
    def _():
        for g in range(GROUPS):
            pltpu.make_async_copy(w_hbm.at[pl.ds(g * GROWS, GROWS)], wv.at[g, pl.ds(0, GROWS)], sems.at[2 * g]).start()
            pltpu.make_async_copy(rt_hbm, wv.at[g, pl.ds(GROWS, E)], sems.at[2 * g + 1]).start()
        greet(x_neighbours() + near)
        own_wd.start()
        for r in first:
            for k in range(2):
                r.start(k)

    @pl.when(step == 1)
    def _():
        for r in first:
            for k in range(2):
                r.last(k)
            r.drain()
        own_wd.wait()
        for r in second:
            for k in range(4):
                r.start(k)

    for tb in range(2):
        def rows(c, tb=tb):
            if x_ref.shape[0] == 2:
                return x_ref[tb, c]
            return x_ref[c, tb]

        def ssq_body(c, acc):
            xf = rows(c).astype(F32)
            return acc + jnp.sum(xf * xf, axis=0, keepdims=True)

        ssq = lax.fori_loop(0, 8, ssq_body, jnp.zeros((1, TB), F32))
        rstd = lax.rsqrt(ssq * (1.0 / D) + NORM_EPS)

        def h_body(c, carry, tb=tb, rstd=rstd):
            xf = rows(c).astype(F32)
            nw = nw_ref[c]
            nw2 = jnp.concatenate([nw, nw], axis=1)
            h[pl.ds(pl.multiple_of(c * 512, 512), 512), tb * TB:(tb + 1) * TB] = (xf * rstd * nw2).astype(BF)
            return carry

        lax.fori_loop(0, 8, h_body, 0)

    slots[...] = jnp.zeros_like(slots)
    idx = jnp.concatenate([idx_ref[0], idx_ref[1]], axis=1)

    def group(g, carry):
        @pl.when(step == 0)
        def _():
            pltpu.make_async_copy(w_hbm.at[pl.ds(g * GROWS, GROWS)], wv.at[g, pl.ds(0, GROWS)], sems.at[2 * g]).wait()
            pltpu.make_async_copy(rt_hbm, wv.at[g, pl.ds(GROWS, E)], sems.at[2 * g + 1]).wait()

        @pl.when(jnp.logical_and(step == 0, g == 3))
        def _():
            for r in first:
                for k in range(2):
                    r.relay(k, k % 2 == 1)

        @pl.when(jnp.logical_and(step >= 1, g == 2))
        def _():
            for tb in range(2):
                ring.relay(2 * step - 2 + tb, tb == 1)

        @pl.when(jnp.logical_and(step == 3, g == 1))
        def _():
            for r in second:
                for k in range(2):
                    r.relay(k, k % 2 == 1)

        @pl.when(jnp.logical_and(step == 3, g == 3))
        def _():
            for r in second:
                for k in range(2, 4):
                    r.relay(k, k % 2 == 1)

        res = jnp.dot(wv[g], h[...], preferred_element_type=F32)
        logits[...] = res[GROWS:]
        for k in range(E // GROUPS):
            u = res[k * 2 * FP:k * 2 * FP + FP]
            v = res[k * 2 * FP + FP:(k + 1) * 2 * FP]
            act = jax.nn.silu(u) * v
            e = g * (E // GROUPS) + k
            for j in range(K):
                slots[j] = jnp.where(idx[j:j + 1] == e, act, slots[j])
        return carry

    lax.fori_loop(0, GROUPS, group, 0)
    for tb in range(2):
        k = 2 * step + tb
        a_buf[k] = slots[:, :, tb * TB:(tb + 1) * TB].astype(BF)
    eids = lax.broadcasted_iota(jnp.int32, (E, 2 * TB), 0)
    chosen = idx[0:1] == eids
    for j in range(1, K):
        chosen = jnp.logical_or(chosen, idx[j:j + 1] == eids)
    lg = jnp.where(chosen, logits[...], -jnp.inf)
    ex = jnp.where(chosen, jnp.exp(lg - jnp.max(lg, axis=0, keepdims=True)), 0.0)
    gates = ex / jnp.sum(ex, axis=0, keepdims=True)
    for tb in range(2):
        g_ref[tb] = gates[:, tb * TB:(tb + 1) * TB]
    for tb in range(2):
        k = 2 * step + tb
        ring.start(k)
        own_a(k).start()

    @pl.when(step == 3)
    def _():
        for k in (6, 7):
            ring.relay(k, k % 2 == 1)
        for k in range(8):
            ring.last(k)
        ring.drain()
        for k in range(8):
            own_a(k).wait()
        for r in second:
            for k in range(4):
                r.last(k)
            r.drain()


def up_proj(x, nw, idx, wd, w, rt, tok_major):
    if tok_major:
        x_spec = pl.BlockSpec((2, 8, 512, TB), lambda i: (i, 0, 0, 0))
    else:
        x_spec = pl.BlockSpec((8, 2, 512, TB), lambda i: (0, i, 0, 0))
    return pl.pallas_call(
        up_kernel,
        grid=(4,),
        out_shape=(jax.ShapeDtypeStruct((8, K, 8 * FP, TB), BF), jax.ShapeDtypeStruct((8, E, TB), F32), jax.ShapeDtypeStruct((E, 512, KP), BF)),
        in_specs=[
            x_spec,
            pl.BlockSpec((8, 512, 128), lambda i: (0, 0, 0)),
            pl.BlockSpec((2, K, TB), lambda i: (i, 0, 0)),
            pl.BlockSpec((512, KP), lambda i: (0, 0)),
            pl.BlockSpec(memory_space=pl.ANY),
            pl.BlockSpec(memory_space=pl.ANY),
        ],
        out_specs=(pl.BlockSpec(memory_space=pl.ANY), pl.BlockSpec((2, E, TB), lambda i: (i, 0, 0)), pl.BlockSpec(memory_space=pl.ANY)),
        scratch_shapes=[
            pltpu.VMEM((GROUPS, GROWS + E, D), BF),
            pltpu.VMEM((D, 2 * TB), BF),
            pltpu.VMEM((K, FP, 2 * TB), F32),
            pltpu.VMEM((E, 2 * TB), F32),
            pltpu.VMEM((8, K, FP, TB), BF),
            pltpu.SemaphoreType.DMA((2 * GROUPS,)),
        ] + X_SEMS + [
            pltpu.SemaphoreType.DMA((2, 3, 2)), pltpu.SemaphoreType.DMA((2, 3, 2)),
            pltpu.SemaphoreType.DMA((2, 3, 4)), pltpu.SemaphoreType.DMA((2, 3, 4)),
            pltpu.SemaphoreType.DMA((9,)),
        ],
        compiler_params=pltpu.CompilerParams(
            vmem_limit_bytes=60 * 1024 * 1024, collective_id=1 if tok_major else 2, has_side_effects=True),
        cost_estimate=pl.CostEstimate(flops=2 * 2832 * D * 2048, bytes_accessed=45_000_000, transcendentals=3_000_000),
        name="up_proj",
    )(x, nw, idx, wd, w, rt)


def down_block(a_ref, idx_ref, g_ref, x_ref, wd_ref, acc, hook):
    idx = jnp.concatenate([idx_ref[0], idx_ref[1]], axis=1).astype(F32).astype(BF)
    acc[...] = jnp.zeros_like(acc)

    def group(g, carry):
        if hook is not None:
            hook(g)
        for k in range(E // GROUPS):
            e = g * (E // GROUPS) + k
            ef = e.astype(F32).astype(BF)
            parts = []
            for tb in range(2):
                sel = jnp.zeros((8 * FP, TB), BF)
                for j in range(K):
                    row = idx[j:j + 1, tb * TB:(tb + 1) * TB]
                    sel = jnp.where(row == ef, a_ref[tb, j], sel)
                parts.append(sel)
            out = jnp.dot(wd_ref[e, :, :8 * FP], jnp.concatenate(parts, axis=1), preferred_element_type=F32)
            gate = jnp.concatenate([g_ref[0, pl.ds(e, 1)], g_ref[1, pl.ds(e, 1)]], axis=1)
            acc[...] += gate * out
        return carry

    lax.fori_loop(0, GROUPS, group, 0)
    xf = lambda tb: x_ref[tb].reshape(512, TB) if len(x_ref.shape) == 4 and x_ref.shape[0] == 2 else x_ref[0, tb]
    return [(xf(tb).astype(F32) + acc[:, tb * TB:(tb + 1) * TB]).astype(BF) for tb in range(2)]


def down_mid_kernel(a_ref, idx_ref, g_ref, x_ref, wd_ref, x_all, acc, o_buf, send_sem, recv_sem, local_sem):
    step = pl.program_id(0)
    f = lax.axis_index("fsdp")
    ring = x_ring(lambda k: o_buf.at[k], lambda owner, k: x_all.at[owner, k], send_sem, recv_sem)

    def own_x(k):
        return pltpu.make_async_copy(o_buf.at[k], x_all.at[f, k], local_sem.at[k])

    @pl.when(step == 0)
    def _():
        greet(x_neighbours())

    def hook(g):
        @pl.when(jnp.logical_and(step >= 2, g == 2))
        def _():
            for tb in range(2):
                ring.relay(2 * step - 4 + tb, tb == 1)

    blocks = down_block(a_ref, idx_ref, g_ref, x_ref, wd_ref, acc, hook)
    for tb in range(2):
        o_buf[2 * step + tb] = blocks[tb]
    for tb in range(2):
        ring.start(2 * step + tb)
        own_x(2 * step + tb).start()

    @pl.when(step == 3)
    def _():
        for k in range(4, 8):
            ring.relay(k, k % 2 == 1)
        for k in range(8):
            ring.last(k)
        ring.drain()
        for k in range(8):
            own_x(k).wait()


def down_last_kernel(a_ref, idx_ref, g_ref, x_ref, wd_ref, o_all, acc, o_buf, psend, precv, local_sem):
    step = pl.program_id(0)
    f = lax.axis_index("fsdp")
    core = f % 2

    @pl.when(step == 0)
    def _():
        greet([{"fsdp": fsdp_at(s, o)} for s, o in PEERS])

    blocks = down_block(a_ref, idx_ref, g_ref, x_ref, wd_ref, acc, None)
    for tb in range(2):
        o_buf[step, tb] = blocks[tb]

    def send(s, o):
        tb = 1 - core if o else core
        return pltpu.make_async_remote_copy(
            src_ref=o_buf.at[(s + 3) % 4, tb], dst_ref=o_all.at[f], send_sem=psend.at[s, o], recv_sem=precv.at[s, o],
            device_id={"fsdp": fsdp_at(s, o)}, device_id_type=MESH)

    for s in range(1, 4):
        @pl.when(step == s - 1)
        def _(s=s):
            send(s, 0).start()
            send(s, 1).start()

    @pl.when(step == 3)
    def _():
        send(0, 1).start()
        mine = pltpu.make_async_copy(o_buf.at[3, core], o_all.at[f], local_sem)
        mine.start()
        for s, o in PEERS:
            source = fsdp_at((4 - s) % 4, o)
            pltpu.make_async_remote_copy(
                src_ref=o_buf.at[0, 0], dst_ref=o_all.at[source], send_sem=psend.at[s, o], recv_sem=precv.at[s, o],
                device_id={"fsdp": source}, device_id_type=MESH).wait_recv()
        for s, o in PEERS:
            send(s, o).wait_send()
        mine.wait()


def down_proj(a, idx, gates, xs_all, wd, tok_major, last):
    if last:
        block = lambda i: lax.rem(lax.axis_index("fsdp") // 2 + 1 + i, 4)
    else:
        block = lambda i: i
    if tok_major:
        x_spec = pl.BlockSpec((2, 1, 512, TB), lambda i: (block(i), lax.axis_index("fsdp"), 0, 0))
    else:
        x_spec = pl.BlockSpec((1, 2, 512, TB), lambda i: (lax.axis_index("fsdp"), block(i), 0, 0))
    return pl.pallas_call(
        down_last_kernel if last else down_mid_kernel,
        grid=(4,),
        out_shape=jax.ShapeDtypeStruct((8, 512, TB) if last else (8, 8, 512, TB), BF),
        in_specs=[
            pl.BlockSpec((2, K, 8 * FP, TB), lambda i: (block(i), 0, 0, 0)),
            pl.BlockSpec((2, K, TB), lambda i: (block(i), 0, 0)),
            pl.BlockSpec((2, E, TB), lambda i: (block(i), 0, 0)),
            x_spec,
            pl.BlockSpec((E, 512, KP), lambda i: (0, 0, 0)),
        ],
        out_specs=pl.BlockSpec(memory_space=pl.ANY),
        scratch_shapes=[pltpu.VMEM((512, 2 * TB), F32)] + (
            [pltpu.VMEM((4, 2, 512, TB), BF), pltpu.SemaphoreType.DMA((4, 2)), pltpu.SemaphoreType.DMA((4, 2)), pltpu.SemaphoreType.DMA]
            if last else [pltpu.VMEM((8, 512, TB), BF)] + X_SEMS + [pltpu.SemaphoreType.DMA((8,))]),
        compiler_params=pltpu.CompilerParams(vmem_limit_bytes=60 * 1024 * 1024, collective_id=4 if last else 3, has_side_effects=True),
        cost_estimate=pl.CostEstimate(flops=2 * 704 * 16 * 512 * 2048, bytes_accessed=30_000_000, transcendentals=0),
        name="down_last" if last else "down_mid",
    )(a, idx, gates, xs_all, wd)


def solution(mesh):
    tok_spec = P(("rep", "ep", "fsdp"), None)
    idx_spec = P(None, ("rep", "ep", "fsdp"), None)
    in_specs = (tok_spec, P(None, None), P(None, None, None), P(None, "ep", None, "fsdp"), P(None, "ep", None, "fsdp"), P(None, "ep", "fsdp", None), idx_spec)

    def local_program(x, norm_w, router_w, w_gate, w_up, w_down, expert_idx):
        layers = norm_w.shape[0]
        pad = jnp.zeros((FP - 86, D), BF)
        rows = [jnp.concatenate([w_gate[l, 0].T, pad, w_up[l, 0].T, pad], axis=0) for l in range(layers)]
        ups = [lax.all_gather(rows[0], "ep", axis=0, tiled=True)]
        xt = x.T.reshape(8, 512, TB)
        wd = jnp.pad(w_down[:, 0], ((0, 0), (0, FP - 86), (0, 0))).reshape(layers, FP, 8, 512).swapaxes(1, 2)
        xt, idx, wd, _ = lax.optimization_barrier((xt, jnp.swapaxes(expert_idx, 1, 2), wd, rows[0]))
        xs_all, idx_all, wd = first_exchange(xt, idx, wd)
        wd = jnp.swapaxes(wd.reshape(layers, 8 * FP, 512), 1, 2)
        wd = jnp.pad(wd, ((0, 0), (0, 0), (0, KP - 8 * FP)))
        for l in range(1, layers):
            nxt, _ = lax.optimization_barrier((rows[l], idx_all))
            ups.append(lax.all_gather(nxt, "ep", axis=0, tiled=True))
        for l in range(layers):
            nw = jnp.broadcast_to(norm_w[l].reshape(8, 512, 1), (8, 512, 128))
            a, gates, wd_all = up_proj(xs_all, nw, idx_all[:, l], wd[l], ups[l], router_w[l].T, l == 0)
            xs_all = down_proj(a, idx_all[:, l], gates, xs_all, wd_all, l == 0, l == layers - 1)
        return xs_all.reshape(D, TB).T

    return jax.shard_map(local_program, mesh=mesh, in_specs=in_specs, out_specs=tok_spec, check_vma=False)
```

```python
import functools

import jax
import jax.numpy as jnp
from jax import lax
from jax.experimental import pallas as pl
from jax.experimental.pallas import tpu as pltpu
from jax.sharding import PartitionSpec as P

NORM_EPS = 1e-5
TB = 256
D = 4096
FP = 88
KP = 768
E = 16
K = 4
GROUPS = 4
GROWS = E // GROUPS * 2 * FP
HALF = 256
BF = jnp.bfloat16
F32 = jnp.float32
MESH = pl.DeviceIdType.MESH
PEERS = [(s, o) for s in range(4) for o in range(2) if (s, o) != (0, 0)]


def fsdp_at(step, other=0):
    f = lax.axis_index("fsdp")
    core = f % 2
    return lax.rem(f // 2 + step, 4) * 2 + (1 - core if other else core)


def greet(devices):
    barrier = pltpu.get_barrier_semaphore()
    for d in devices:
        pl.semaphore_signal(barrier, inc=1, device_id=d, device_id_type=MESH)
    pl.semaphore_wait(barrier, len(devices))


class Ring:
    def __init__(self, pos, dev, own, place, chunks, send_sem, recv_sem, partner=None):
        self.pos, self.dev, self.own, self.place, self.chunks = pos, dev, own, place, chunks
        self.send_sem, self.recv_sem, self.partner = send_sem, recv_sem, partner

    def at(self, step):
        return lax.rem(self.pos + step, 4)

    def copy(self, kind, k, src, dst, device):
        return pltpu.make_async_remote_copy(
            src_ref=src, dst_ref=dst, send_sem=self.send_sem.at[kind, k], recv_sem=self.recv_sem.at[kind, k],
            device_id=device, device_id_type=MESH)

    def own_copies(self, k):
        mine = self.place(self.pos, k)
        out = [self.copy(0, k, self.own(k), mine, self.dev(self.at(1))), self.copy(1, k, self.own(k), mine, self.dev(self.at(3)))]
        if self.partner is not None:
            out.append(self.copy(3, k, self.own(k), mine, self.partner))
        return out

    def onward(self, k, odd):
        source, target = (self.at(1), self.at(3)) if odd else (self.at(3), self.at(1))
        ref = self.place(source, k)
        return self.copy(2, k, ref, ref, self.dev(target))

    def across(self, kind, k):
        ref = self.place(self.at({4: 3, 5: 1, 6: 2}[kind]), k)
        return self.copy(kind, k, ref, ref, self.partner)

    def arrived(self, kind, k, step, other=0):
        ref = self.place(self.at(step), k, 1) if other else self.place(self.at(step), k)
        self.copy(kind, k, ref, ref, self.dev(self.at(1))).wait_recv()

    def start(self, k):
        for c in self.own_copies(k):
            c.start()

    def relay(self, k, odd):
        self.arrived(0, k, 3)
        if not odd:
            self.onward(k, odd).start()
        if self.partner is not None:
            self.across(4, k).start()
        self.arrived(1, k, 1)
        if odd:
            self.onward(k, odd).start()
        if self.partner is not None:
            self.across(5, k).start()

    def last(self, k):
        self.arrived(2, k, 2)
        if self.partner is not None:
            self.across(6, k).start()

    def drain(self):
        for k in range(self.chunks):
            if self.partner is not None:
                for kind, step in ((3, 0), (4, 3), (5, 1), (6, 2)):
                    self.arrived(kind, k, step, 1)
            for c in self.own_copies(k):
                c.wait_send()
            self.onward(k, k % 2 == 1).wait_send()
            if self.partner is not None:
                for kind in (4, 5, 6):
                    self.across(kind, k).wait_send()


def x_ring(own, place, send_sem, recv_sem):
    f = lax.axis_index("fsdp")
    core = f % 2

    def where(p, k, other=0):
        return place(p * 2 + (1 - core if other else core), k)

    return Ring(f // 2, lambda p: {"fsdp": p * 2 + core}, own, where, 8, send_sem, recv_sem, {"fsdp": fsdp_at(0, 1)})


X_SEMS = [pltpu.SemaphoreType.DMA((7, 8)), pltpu.SemaphoreType.DMA((7, 8))]


def x_neighbours():
    return [{"fsdp": fsdp_at(1)}, {"fsdp": fsdp_at(3)}, {"fsdp": fsdp_at(0, 1)}]


def first_kernel(x_ref, idx_ref, wd_ref, x_all, idx_all, wd_all, send_sem, recv_sem, local_sem, psend, precv):
    f = lax.axis_index("fsdp")
    greet([{"fsdp": fsdp_at(s, o)} for s, o in PEERS])
    ring = x_ring(lambda k: x_ref.at[k], lambda owner, k: x_all.at[owner, k], send_sem, recv_sem)
    locals_ = [
        pltpu.make_async_copy(x_ref, x_all.at[f], local_sem.at[0]),
        pltpu.make_async_copy(idx_ref, idx_all.at[f], local_sem.at[1]),
        pltpu.make_async_copy(wd_ref.at[:, f], wd_all.at[:, f], local_sem.at[2]),
    ]
    for c in locals_:
        c.start()
    small = []
    for p, (s, o) in enumerate(PEERS):
        peer = fsdp_at(s, o)
        small.append(pltpu.make_async_remote_copy(
            src_ref=idx_ref, dst_ref=idx_all.at[f], send_sem=psend.at[0, p], recv_sem=precv.at[0, p],
            device_id={"fsdp": peer}, device_id_type=MESH))
        small.append(pltpu.make_async_remote_copy(
            src_ref=wd_ref.at[:, peer], dst_ref=wd_all.at[:, f], send_sem=psend.at[1, p], recv_sem=precv.at[1, p],
            device_id={"fsdp": peer}, device_id_type=MESH))
    for c in small:
        c.start()
    for k in range(8):
        ring.start(k)
    for k in range(8):
        ring.relay(k, k % 2 == 1)
    for k in range(8):
        ring.last(k)
    ring.drain()
    for p, (s, o) in enumerate(PEERS):
        source = fsdp_at((4 - s) % 4, o)
        for kind, (src, dst) in enumerate(((idx_ref, idx_all.at[source]), (wd_ref.at[:, 0], wd_all.at[:, source]))):
            pltpu.make_async_remote_copy(
                src_ref=src, dst_ref=dst, send_sem=psend.at[kind, p], recv_sem=precv.at[kind, p],
                device_id={"fsdp": source}, device_id_type=MESH).wait_recv()
    for c in small:
        c.wait_send()
    for c in locals_:
        c.wait()


def first_exchange(xt, idx, wd):
    return pl.pallas_call(
        first_kernel,
        out_shape=(jax.ShapeDtypeStruct((8, 8, 512, TB), BF), jax.ShapeDtypeStruct((8, 2, K, TB), jnp.int32), jax.ShapeDtypeStruct((2, 8, FP, 512), BF)),
        in_specs=[pl.BlockSpec(memory_space=pltpu.VMEM)] * 3,
        out_specs=[pl.BlockSpec(memory_space=pl.ANY)] * 3,
        scratch_shapes=X_SEMS + [pltpu.SemaphoreType.DMA((3,)), pltpu.SemaphoreType.DMA((2, 7)), pltpu.SemaphoreType.DMA((2, 7))],
        compiler_params=pltpu.CompilerParams(collective_id=0, has_side_effects=True),
        cost_estimate=pl.CostEstimate(flops=70_000_000_000, bytes_accessed=16_000_000, transcendentals=0),
        name="first_exchange",
    )(xt, idx, wd)


def wd_rings(wd_ref, wd_all, send1, recv1, send2, recv2):
    e = lax.axis_index("ep")
    z, y = e // 4, e % 4
    on_y = lambda p: {"ep": z * 4 + p}
    on_z = lambda p: {"ep": p * 4 + y}
    rows = lambda b, k: pl.ds(b * HALF + k * (HALF // 2), HALF // 2)
    first = [
        Ring(y, on_y, lambda k: wd_ref.at[rows(0, k)], lambda p, k: wd_all.at[z * 4 + p, rows(0, k)], 2, send1.at[0], recv1.at[0]),
        Ring(z, on_z, lambda k: wd_ref.at[rows(1, k)], lambda p, k: wd_all.at[p * 4 + y, rows(1, k)], 2, send1.at[1], recv1.at[1]),
    ]
    by_z = lambda p, k: wd_all.at[p * 4 + k, pl.ds(0, HALF)]
    by_y = lambda p, k: wd_all.at[k * 4 + p, pl.ds(HALF, HALF)]
    second = [
        Ring(z, on_z, lambda k: by_z(z, k), by_z, 4, send2.at[0], recv2.at[0]),
        Ring(y, on_y, lambda k: by_y(y, k), by_y, 4, send2.at[1], recv2.at[1]),
    ]
    near = [on_y(lax.rem(y + 1, 4)), on_y(lax.rem(y + 3, 4)), on_z(lax.rem(z + 1, 4)), on_z(lax.rem(z + 3, 4))]
    return first, second, near


def norm_kernel(x_ref, nw_ref, h_ref):
    for tb in range(2):
        def rows(c, tb=tb):
            if x_ref.shape[0] == 2:
                return x_ref[tb, c]
            return x_ref[c, tb]

        def ssq_body(c, acc):
            xf = rows(c).astype(F32)
            return acc + jnp.sum(xf * xf, axis=0, keepdims=True)

        ssq = lax.fori_loop(0, 8, ssq_body, jnp.zeros((1, TB), F32))
        rstd = lax.rsqrt(ssq * (1.0 / D) + NORM_EPS)

        def h_body(c, carry, tb=tb, rstd=rstd):
            xf = rows(c).astype(F32)
            nw = nw_ref[c]
            nw2 = jnp.concatenate([nw, nw], axis=1)
            h_ref[0, pl.ds(pl.multiple_of(c * 512, 512), 512), tb * TB:(tb + 1) * TB] = (xf * rstd * nw2).astype(BF)
            return carry

        lax.fori_loop(0, 8, h_body, 0)


def norm(x, nw, tok_major):
    if tok_major:
        x_spec = pl.BlockSpec((2, 8, 512, TB), lambda i: (i, 0, 0, 0))
    else:
        x_spec = pl.BlockSpec((8, 2, 512, TB), lambda i: (0, i, 0, 0))
    return pl.pallas_call(
        norm_kernel,
        grid=(4,),
        out_shape=jax.ShapeDtypeStruct((4, D, 2 * TB), BF),
        in_specs=[x_spec, pl.BlockSpec((8, 512, 128), lambda i: (0, 0, 0))],
        out_specs=pl.BlockSpec((1, D, 2 * TB), lambda i: (i, 0, 0)),
        compiler_params=pltpu.CompilerParams(vmem_limit_bytes=40 * 1024 * 1024),
        cost_estimate=pl.CostEstimate(flops=20_000_000_000, bytes_accessed=34_000_000, transcendentals=0),
        name="norm",
    )(x, nw)


def up_kernel(
    h_ref, idx_ref, wd_ref, w_hbm, rt_hbm, a_all, g_ref, wd_all,
    wv, slots, logits, a_buf, sems, send_sem, recv_sem, send1, recv1, send2, recv2, local_sem,
):
    step = pl.program_id(0)
    f = lax.axis_index("fsdp")
    mine = lambda owner: pl.ds(pl.multiple_of(owner * FP, 8), FP)
    ring = x_ring(lambda k: a_buf.at[k], lambda owner, k: a_all.at[k, :, mine(owner)], send_sem, recv_sem)
    first, second, near = wd_rings(wd_ref, wd_all, send1, recv1, send2, recv2)
    own_wd = pltpu.make_async_copy(wd_ref, wd_all.at[lax.axis_index("ep")], local_sem.at[8])

    def own_a(k):
        return pltpu.make_async_copy(a_buf.at[k], a_all.at[k, :, mine(f)], local_sem.at[k])

    @pl.when(step == 0)
    def _():
        for g in range(GROUPS):
            pltpu.make_async_copy(w_hbm.at[pl.ds(g * GROWS, GROWS)], wv.at[g, pl.ds(0, GROWS)], sems.at[2 * g]).start()
            pltpu.make_async_copy(rt_hbm, wv.at[g, pl.ds(GROWS, E)], sems.at[2 * g + 1]).start()
        greet(x_neighbours() + near)
        own_wd.start()
        for r in first:
            for k in range(2):
                r.start(k)

    slots[...] = jnp.zeros_like(slots)
    idx = jnp.concatenate([idx_ref[0], idx_ref[1]], axis=1)

    def group(g, carry):
        @pl.when(step == 0)
        def _():
            pltpu.make_async_copy(w_hbm.at[pl.ds(g * GROWS, GROWS)], wv.at[g, pl.ds(0, GROWS)], sems.at[2 * g]).wait()
            pltpu.make_async_copy(rt_hbm, wv.at[g, pl.ds(GROWS, E)], sems.at[2 * g + 1]).wait()

        @pl.when(jnp.logical_and(step >= 1, g == 3))
        def _():
            for tb in range(2):
                ring.relay(2 * step - 2 + tb, tb == 1)

        tick = step * GROUPS + g

        @pl.when(tick == 3)
        def _():
            for k in range(2):
                for r in first:
                    r.relay(k, k % 2 == 1)

        @pl.when(tick == 5)
        def _():
            for r in first:
                for k in range(2):
                    r.last(k)
                r.drain()
            own_wd.wait()
            for k in range(4):
                for r in second:
                    r.start(k)

        for k, t in enumerate((9, 12, 15)):
            @pl.when(tick == t)
            def _(k=k):
                for r in second:
                    r.relay(k, k % 2 == 1)

        res = jnp.dot(wv[g], h_ref[0], preferred_element_type=F32)
        logits[...] = res[GROWS:]
        for k in range(E // GROUPS):
            u = res[k * 2 * FP:k * 2 * FP + FP]
            v = res[k * 2 * FP + FP:(k + 1) * 2 * FP]
            act = jax.nn.silu(u) * v
            e = g * (E // GROUPS) + k
            for j in range(K):
                slots[j] = jnp.where(idx[j:j + 1] == e, act, slots[j])
        return carry

    lax.fori_loop(0, GROUPS, group, 0)
    for tb in range(2):
        k = 2 * step + tb
        a_buf[k] = slots[:, :, tb * TB:(tb + 1) * TB].astype(BF)
    eids = lax.broadcasted_iota(jnp.int32, (E, 2 * TB), 0)
    chosen = idx[0:1] == eids
    for j in range(1, K):
        chosen = jnp.logical_or(chosen, idx[j:j + 1] == eids)
    lg = jnp.where(chosen, logits[...], -jnp.inf)
    ex = jnp.where(chosen, jnp.exp(lg - jnp.max(lg, axis=0, keepdims=True)), 0.0)
    gates = ex / jnp.sum(ex, axis=0, keepdims=True)
    for tb in range(2):
        g_ref[tb] = gates[:, tb * TB:(tb + 1) * TB]
    for tb in range(2):
        k = 2 * step + tb
        ring.start(k)
        own_a(k).start()

    @pl.when(step == 3)
    def _():
        for r in second:
            r.relay(3, True)
        for k in (6, 7):
            ring.relay(k, k % 2 == 1)
        for k in range(8):
            ring.last(k)
        ring.drain()
        for k in range(8):
            own_a(k).wait()
        for r in second:
            for k in range(4):
                r.last(k)
            r.drain()


def up_proj(h, idx, wd, w, rt, layer):
    return pl.pallas_call(
        up_kernel,
        grid=(4,),
        out_shape=(jax.ShapeDtypeStruct((8, K, 8 * FP, TB), BF), jax.ShapeDtypeStruct((8, E, TB), F32), jax.ShapeDtypeStruct((E, 512, KP), BF)),
        in_specs=[
            pl.BlockSpec((1, D, 2 * TB), lambda i: (i, 0, 0)),
            pl.BlockSpec((2, K, TB), lambda i: (i, 0, 0)),
            pl.BlockSpec((512, KP), lambda i: (0, 0)),
            pl.BlockSpec(memory_space=pl.ANY),
            pl.BlockSpec(memory_space=pl.ANY),
        ],
        out_specs=(pl.BlockSpec(memory_space=pl.ANY), pl.BlockSpec((2, E, TB), lambda i: (i, 0, 0)), pl.BlockSpec(memory_space=pl.ANY)),
        scratch_shapes=[
            pltpu.VMEM((GROUPS, GROWS + E, D), BF),
            pltpu.VMEM((K, FP, 2 * TB), F32),
            pltpu.VMEM((E, 2 * TB), F32),
            pltpu.VMEM((8, K, FP, TB), BF),
            pltpu.SemaphoreType.DMA((2 * GROUPS,)),
        ] + X_SEMS + [
            pltpu.SemaphoreType.DMA((2, 3, 2)), pltpu.SemaphoreType.DMA((2, 3, 2)),
            pltpu.SemaphoreType.DMA((2, 3, 4)), pltpu.SemaphoreType.DMA((2, 3, 4)),
            pltpu.SemaphoreType.DMA((9,)),
        ],
        compiler_params=pltpu.CompilerParams(
            vmem_limit_bytes=60 * 1024 * 1024, collective_id=1, has_side_effects=True),
        cost_estimate=pl.CostEstimate(flops=2 * 2832 * D * 2048, bytes_accessed=45_000_000, transcendentals=3_000_000),
        name="up_proj",
    )(h, idx, wd, w, rt)


def down_block(a_ref, idx_ref, g_ref, x_ref, wd_ref, acc, hook):
    idx = jnp.concatenate([idx_ref[0], idx_ref[1]], axis=1).astype(F32).astype(BF)
    acc[...] = jnp.zeros_like(acc)

    def group(g, carry):
        if hook is not None:
            hook(g)
        for k in range(E // GROUPS):
            e = g * (E // GROUPS) + k
            ef = e.astype(F32).astype(BF)
            parts = []
            for tb in range(2):
                sel = jnp.zeros((8 * FP, TB), BF)
                for j in range(K):
                    row = idx[j:j + 1, tb * TB:(tb + 1) * TB]
                    sel = jnp.where(row == ef, a_ref[tb, j], sel)
                parts.append(sel)
            out = jnp.dot(wd_ref[e, :, :8 * FP], jnp.concatenate(parts, axis=1), preferred_element_type=F32)
            gate = jnp.concatenate([g_ref[0, pl.ds(e, 1)], g_ref[1, pl.ds(e, 1)]], axis=1)
            acc[...] += gate * out
        return carry

    lax.fori_loop(0, GROUPS, group, 0)
    xf = lambda tb: x_ref[tb].reshape(512, TB) if len(x_ref.shape) == 4 and x_ref.shape[0] == 2 else x_ref[0, tb]
    return [(xf(tb).astype(F32) + acc[:, tb * TB:(tb + 1) * TB]).astype(BF) for tb in range(2)]


def down_mid_kernel(a_ref, idx_ref, g_ref, x_ref, wd_ref, x_all, acc, o_buf, send_sem, recv_sem, local_sem):
    step = pl.program_id(0)
    f = lax.axis_index("fsdp")
    ring = x_ring(lambda k: o_buf.at[k], lambda owner, k: x_all.at[owner, k], send_sem, recv_sem)

    def own_x(k):
        return pltpu.make_async_copy(o_buf.at[k], x_all.at[f, k], local_sem.at[k])

    @pl.when(step == 0)
    def _():
        greet(x_neighbours())

    def hook(g):
        @pl.when(jnp.logical_and(step >= 2, g == 2))
        def _():
            for tb in range(2):
                ring.relay(2 * step - 4 + tb, tb == 1)

    blocks = down_block(a_ref, idx_ref, g_ref, x_ref, wd_ref, acc, hook)
    for tb in range(2):
        o_buf[2 * step + tb] = blocks[tb]
    for tb in range(2):
        ring.start(2 * step + tb)
        own_x(2 * step + tb).start()

    @pl.when(step == 3)
    def _():
        for k in range(4, 8):
            ring.relay(k, k % 2 == 1)
        for k in range(8):
            ring.last(k)
        ring.drain()
        for k in range(8):
            own_x(k).wait()


def down_last_kernel(a_ref, idx_ref, g_ref, x_ref, wd_ref, o_all, acc, o_buf, psend, precv, local_sem):
    step = pl.program_id(0)
    f = lax.axis_index("fsdp")
    core = f % 2

    @pl.when(step == 0)
    def _():
        greet([{"fsdp": fsdp_at(s, o)} for s, o in PEERS])

    blocks = down_block(a_ref, idx_ref, g_ref, x_ref, wd_ref, acc, None)
    for tb in range(2):
        o_buf[step, tb] = blocks[tb]

    def send(s, o):
        tb = 1 - core if o else core
        return pltpu.make_async_remote_copy(
            src_ref=o_buf.at[(s + 3) % 4, tb], dst_ref=o_all.at[f], send_sem=psend.at[s, o], recv_sem=precv.at[s, o],
            device_id={"fsdp": fsdp_at(s, o)}, device_id_type=MESH)

    for s in range(1, 4):
        @pl.when(step == s - 1)
        def _(s=s):
            send(s, 0).start()
            send(s, 1).start()

    @pl.when(step == 3)
    def _():
        send(0, 1).start()
        mine = pltpu.make_async_copy(o_buf.at[3, core], o_all.at[f], local_sem)
        mine.start()
        for s, o in PEERS:
            source = fsdp_at((4 - s) % 4, o)
            pltpu.make_async_remote_copy(
                src_ref=o_buf.at[0, 0], dst_ref=o_all.at[source], send_sem=psend.at[s, o], recv_sem=precv.at[s, o],
                device_id={"fsdp": source}, device_id_type=MESH).wait_recv()
        for s, o in PEERS:
            send(s, o).wait_send()
        mine.wait()


def down_proj(a, idx, gates, xs_all, wd, tok_major, last):
    if last:
        block = lambda i: lax.rem(lax.axis_index("fsdp") // 2 + 1 + i, 4)
    else:
        block = lambda i: i
    if tok_major:
        x_spec = pl.BlockSpec((2, 1, 512, TB), lambda i: (block(i), lax.axis_index("fsdp"), 0, 0))
    else:
        x_spec = pl.BlockSpec((1, 2, 512, TB), lambda i: (lax.axis_index("fsdp"), block(i), 0, 0))
    return pl.pallas_call(
        down_last_kernel if last else down_mid_kernel,
        grid=(4,),
        out_shape=jax.ShapeDtypeStruct((8, 512, TB) if last else (8, 8, 512, TB), BF),
        in_specs=[
            pl.BlockSpec((2, K, 8 * FP, TB), lambda i: (block(i), 0, 0, 0)),
            pl.BlockSpec((2, K, TB), lambda i: (block(i), 0, 0)),
            pl.BlockSpec((2, E, TB), lambda i: (block(i), 0, 0)),
            x_spec,
            pl.BlockSpec((E, 512, KP), lambda i: (0, 0, 0)),
        ],
        out_specs=pl.BlockSpec(memory_space=pl.ANY),
        scratch_shapes=[pltpu.VMEM((512, 2 * TB), F32)] + (
            [pltpu.VMEM((4, 2, 512, TB), BF), pltpu.SemaphoreType.DMA((4, 2)), pltpu.SemaphoreType.DMA((4, 2)), pltpu.SemaphoreType.DMA]
            if last else [pltpu.VMEM((8, 512, TB), BF)] + X_SEMS + [pltpu.SemaphoreType.DMA((8,))]),
        compiler_params=pltpu.CompilerParams(vmem_limit_bytes=60 * 1024 * 1024, collective_id=4 if last else 3, has_side_effects=True),
        cost_estimate=pl.CostEstimate(flops=2 * 704 * 16 * 512 * 2048, bytes_accessed=30_000_000, transcendentals=0),
        name="down_last" if last else "down_mid",
    )(a, idx, gates, xs_all, wd)


def solution(mesh):
    tok_spec = P(("rep", "ep", "fsdp"), None)
    idx_spec = P(None, ("rep", "ep", "fsdp"), None)
    in_specs = (tok_spec, P(None, None), P(None, None, None), P(None, "ep", None, "fsdp"), P(None, "ep", None, "fsdp"), P(None, "ep", "fsdp", None), idx_spec)

    def local_program(x, norm_w, router_w, w_gate, w_up, w_down, expert_idx):
        layers = norm_w.shape[0]
        pad = jnp.zeros((FP - 86, D), BF)

        def pack(gate, up):
            return jnp.concatenate([gate.T, pad, up.T, pad], axis=0)

        rows = pack(w_gate[0, 0], w_up[0, 0])
        ups = [lax.all_gather(rows, "ep", axis=0, tiled=True)]
        xt = x.T.reshape(8, 512, TB)
        wd = jnp.pad(w_down[:, 0], ((0, 0), (0, FP - 86), (0, 0))).reshape(layers, FP, 8, 512).swapaxes(1, 2)
        xt, idx, wd, _ = lax.optimization_barrier((xt, jnp.swapaxes(expert_idx, 1, 2), wd, rows))
        xs_all, idx_all, wd = first_exchange(xt, idx, wd)
        wd = jnp.swapaxes(wd.reshape(layers, 8 * FP, 512), 1, 2)
        wd = jnp.pad(wd, ((0, 0), (0, 0), (0, KP - 8 * FP)))
        gates_w, ups_w, _ = lax.optimization_barrier((w_gate, w_up, idx_all))
        for l in range(1, layers):
            ups.append(lax.all_gather(pack(gates_w[l, 0], ups_w[l, 0]), "ep", axis=0, tiled=True))
        for l in range(layers):
            nw = jnp.broadcast_to(norm_w[l].reshape(8, 512, 1), (8, 512, 128))
            h = norm(xs_all, nw, l == 0)
            a, gates, wd_all = up_proj(h, idx_all[:, l], wd[l], ups[l], router_w[l].T, l)
            xs_all = down_proj(a, idx_all[:, l], gates, xs_all, wd_all, l == 0, l == layers - 1)
        return xs_all.reshape(D, TB).T

    return jax.shard_map(local_program, mesh=mesh, in_specs=in_specs, out_specs=tok_spec, check_vma=False)
```

```python
import jax
import jax.numpy as jnp
from jax import lax
from jax.experimental import pallas as pl
from jax.experimental.pallas import tpu as pltpu
from jax.sharding import PartitionSpec as P

NORM_EPS = 1e-5
TB = 256
TB2 = 512
NB = 8
D = 4096
DS = 512
F = 86
FP = 88
FA = 48
RA = 96
RB = 80
RE = 176
KP = 768
E = 16
K = 4
STEPS = 4
GE = 4
GROWS = GE * RE
BF = jnp.bfloat16
F32 = jnp.float32
MESH = pl.DeviceIdType.MESH
DMA = pltpu.SemaphoreType.DMA
ANY = pl.BlockSpec(memory_space=pl.ANY)
IN_VMEM = pl.BlockSpec(memory_space=pltpu.VMEM)
PEERS = [(s, o) for s in range(4) for o in range(2) if s + o]


def shape(dims, dtype=BF):
    return jax.ShapeDtypeStruct(dims, dtype)


def params(collective_id):
    return pltpu.CompilerParams(vmem_limit_bytes=62_000_000, collective_id=collective_id, has_side_effects=True)


def cost(micros):
    return pl.CostEstimate(flops=micros * 1_000_000_000, bytes_accessed=10_000_000, transcendentals=0)


def remote(src, dst, send_sem, recv_sem, device):
    return pltpu.make_async_remote_copy(src_ref=src, dst_ref=dst, send_sem=send_sem, recv_sem=recv_sem, device_id=device, device_id_type=MESH)


def fsdp_at(step, other=0):
    f = lax.axis_index("fsdp")
    core = f % 2
    return lax.rem(f // 2 + step, 4) * 2 + (1 - core if other else core)


def greet(devices):
    barrier = pltpu.get_barrier_semaphore()
    for d in devices:
        pl.semaphore_signal(barrier, inc=1, device_id=d, device_id_type=MESH)
    pl.semaphore_wait(barrier, len(devices))


class Ring:
    def __init__(self, pos, dev, own, place, chunks, send_sem, recv_sem, partner=None):
        self.pos, self.dev, self.own, self.place, self.chunks = pos, dev, own, place, chunks
        self.send_sem, self.recv_sem, self.partner = send_sem, recv_sem, partner
        self.right, self.left, self.far = [lax.rem(pos + s, 4) for s in (1, 3, 2)]

    def copy(self, kind, k, src, dst, device):
        return remote(src, dst, self.send_sem.at[kind, k], self.recv_sem.at[kind, k], device)

    def own_copies(self, k):
        mine = self.place(self.pos, k)
        out = [self.copy(0, k, self.own(k), mine, self.dev(self.right)), self.copy(1, k, self.own(k), mine, self.dev(self.left))]
        if self.partner is not None:
            out.append(self.copy(3, k, self.own(k), mine, self.partner))
        return out

    def onward(self, k, odd):
        source, target = (self.right, self.left) if odd else (self.left, self.right)
        ref = self.place(source, k)
        return self.copy(2, k, ref, ref, self.dev(target))

    def across(self, kind, k):
        ref = self.place({4: self.left, 5: self.right, 6: self.far}[kind], k)
        return self.copy(kind, k, ref, ref, self.partner)

    def arrived(self, kind, k, pos, *other):
        ref = self.place(pos, k, *other)
        self.copy(kind, k, ref, ref, self.dev(self.right)).wait_recv()

    def start(self, k):
        for c in self.own_copies(k):
            c.start()

    def relay(self, k, odd):
        for kind, pos, onward in ((0, self.left, not odd), (1, self.right, odd)):
            self.arrived(kind, k, pos)
            if onward:
                self.onward(k, odd).start()
            if self.partner is not None:
                self.across(4 + kind, k).start()

    def last(self, k):
        self.arrived(2, k, self.far)
        if self.partner is not None:
            self.across(6, k).start()

    def from_partner(self, k):
        for kind, pos in ((3, self.pos), (4, self.left), (5, self.right), (6, self.far)):
            self.arrived(kind, k, pos, 1)

    def drain(self):
        for k in range(self.chunks):
            for c in self.own_copies(k):
                c.wait_send()
            self.onward(k, k % 2 == 1).wait_send()
            if self.partner is not None:
                for kind in (4, 5, 6):
                    self.across(kind, k).wait_send()


def x_ring(own, place, send_sem, recv_sem):
    f = lax.axis_index("fsdp")
    core = f % 2

    def where(p, k, other=0):
        return place(p * 2 + (1 - core if other else core), k)

    return Ring(f // 2, lambda p: {"fsdp": p * 2 + core}, own, where, NB, send_sem, recv_sem, {"fsdp": fsdp_at(0, 1)})


X_SEMS = [DMA((7, NB)), DMA((7, NB))]
FIRST_SEMS = [DMA((2, 3, 2)), DMA((2, 3, 2))]
SECOND_SEMS = [DMA((2, 3, 4)), DMA((2, 3, 4))]


def x_neighbours():
    return [{"fsdp": fsdp_at(1)}, {"fsdp": fsdp_at(3)}, {"fsdp": fsdp_at(0, 1)}]


def yz():
    e = lax.axis_index("ep")
    z, y = e // 4, e % 4
    return z, y, (lambda p: {"ep": p * 4 + y}), (lambda p: {"ep": z * 4 + p})


def yz_neighbours():
    z, y, on_z, on_y = yz()
    return [f(lax.rem(p + s, 4)) for f, p in ((on_z, z), (on_y, y)) for s in (1, 3)]


def cut(ref, lanes, half, chunk=None):
    size = ref.shape[1 if lanes else 0] // 2
    span = pl.ds(half * size, size) if chunk is None else pl.ds(half * size + chunk * (size // 2), size // 2)
    return ref.at[:, span] if lanes else ref.at[span]


def first_rings(own, full, lanes, sems):
    z, y, on_z, on_y = yz()
    send, recv = sems
    return [
        Ring(y, on_y, lambda k: cut(own, lanes, 0, k), lambda p, k: cut(full.at[z * 4 + p], lanes, 0, k), 2, send.at[0], recv.at[0]),
        Ring(z, on_z, lambda k: cut(own, lanes, 1, k), lambda p, k: cut(full.at[p * 4 + y], lanes, 1, k), 2, send.at[1], recv.at[1]),
    ]


def second_rings(full, lanes, sems):
    z, y, on_z, on_y = yz()
    send, recv = sems
    by_z = lambda p, k: cut(full.at[p * 4 + k], lanes, 0)
    by_y = lambda p, k: cut(full.at[k * 4 + p], lanes, 1)
    return [
        Ring(z, on_z, lambda k: by_z(z, k), by_z, 4, send.at[0], recv.at[0]),
        Ring(y, on_y, lambda k: by_y(y, k), by_y, 4, send.at[1], recv.at[1]),
    ]


def start(rings):
    for k in range(rings[0].chunks):
        for r in rings:
            r.start(k)


def relay(rings, k):
    for r in rings:
        r.relay(k, k % 2 == 1)


def finish(rings):
    for r in rings:
        for k in range(r.chunks):
            r.last(k)
        r.drain()


def norm_block(view, nw_ref, stage, h_stage, h_out, sems, tok_major):
    load = pltpu.make_async_copy(view, stage, sems.at[0])
    load.start()
    load.wait()
    for tb in range(2):
        def rows(c, tb=tb):
            return (stage[tb, c] if tok_major else stage[c, tb]).astype(F32)

        def ssq_body(c, acc):
            xf = rows(c)
            return acc + jnp.sum(xf * xf, axis=0, keepdims=True)

        ssq = lax.fori_loop(0, NB, ssq_body, jnp.zeros((1, TB), F32))
        rstd = lax.rsqrt(ssq * (1.0 / D) + NORM_EPS)

        def h_body(c, carry, tb=tb, rstd=rstd):
            nw = nw_ref[c]
            nw2 = jnp.concatenate([nw, nw], axis=1)
            h_stage[pl.ds(pl.multiple_of(c * DS, DS), DS), tb * TB:(tb + 1) * TB] = (rows(c) * rstd * nw2).astype(BF)
            return carry

        lax.fori_loop(0, NB, h_body, 0)
    store = pltpu.make_async_copy(h_stage, h_out, sems.at[1])
    store.start()
    store.wait()


def first_kernel(
    x_ref, nw_ref, w_ref, idx_ref, wd_ref, x_all, h_all, w_all, idx_all, wd_all, wd_next,
    stage, h_stage, wd_in, wd_out, local_sem, norm_sem, small_send, small_recv, *sems,
):
    f, e = lax.axis_index("fsdp"), lax.axis_index("ep")
    greet([{"fsdp": fsdp_at(s, o)} for s, o in PEERS] + yz_neighbours())
    ring = x_ring(lambda k: x_ref.at[k], lambda owner, k: x_all.at[owner, k], *sems[:2])
    w_first = first_rings(w_ref, w_all, True, sems[2:4])
    w_second = second_rings(w_all, True, sems[4:6])
    d_first = first_rings(wd_out.at[0], wd_all, False, sems[6:])
    own = [pltpu.make_async_copy(src, dst, local_sem.at[i])
           for i, (src, dst) in enumerate((
               (w_ref, w_all.at[e]), (x_ref, x_all.at[f]), (wd_ref.at[:, f], wd_in.at[:, f]), (idx_ref, idx_all.at[f])))]
    after = [pltpu.make_async_copy(wd_out.at[0], wd_all.at[e], local_sem.at[4]), pltpu.make_async_copy(wd_out.at[1], wd_next, local_sem.at[5])]
    small = []
    for p, (s, o) in enumerate(PEERS):
        peer = fsdp_at(s, o)
        small.append(remote(wd_ref.at[:, peer], wd_in.at[:, f], small_send.at[0, p], small_recv.at[0, p], {"fsdp": peer}))
        small.append(remote(idx_ref, idx_all.at[f], small_send.at[1, p], small_recv.at[1, p], {"fsdp": peer}))
    start(w_first)
    for c in small + own:
        c.start()
    for k in range(NB):
        ring.start(k)
    for p, (s, o) in enumerate(PEERS):
        source = fsdp_at((4 - s) % 4, o)
        remote(wd_ref.at[:, 0], wd_in.at[:, source], small_send.at[0, p], small_recv.at[0, p], {"fsdp": source}).wait_recv()
        remote(idx_ref, idx_all.at[source], small_send.at[1, p], small_recv.at[1, p], {"fsdp": source}).wait_recv()
    for c in own[2:]:
        c.wait()
    for l in range(2):
        wd_out[l, :, :NB * FP] = jnp.swapaxes(wd_in[l].reshape(NB * FP, DS), 0, 1)
        wd_out[l, :, NB * FP:] = jnp.zeros((DS, KP - NB * FP), BF)
    relay(w_first, 0)
    for k in range(NB):
        ring.relay(k, k % 2 == 1)
        if k == 0:
            relay(w_first, 1)
            for c in after:
                c.start()
            start(d_first)
        if k == 3:
            finish(w_first)
            own[0].wait()
            start(w_second)
        if k in (5, 6):
            relay(d_first, k - 5)
    for k in range(NB):
        ring.last(k)
        if k in (0, 4):
            relay(w_second, k // 4)
    for k in range(NB):
        ring.from_partner(k)
    own[1].wait()
    for i in range(STEPS):
        if i < 2:
            relay(w_second, i + 2)
        norm_block(x_all.at[pl.ds(2 * i, 2)], nw_ref, stage, h_stage, h_all.at[i], norm_sem, True)
    finish(d_first)
    for c in after:
        c.wait()
    finish(w_second)
    ring.drain()
    for c in small:
        c.wait_send()


def first_exchange(xt, nw, w, idx, wd):
    return pl.pallas_call(
        first_kernel,
        out_shape=(
            shape((NB, NB, DS, TB)), shape((STEPS, D, TB2)), shape((E,) + w.shape), shape((NB,) + idx.shape, jnp.int32),
            shape((E, DS, KP)), shape((DS, KP))),
        in_specs=[IN_VMEM] * 5,
        out_specs=[ANY] * 6,
        scratch_shapes=[
            pltpu.VMEM((2, NB, DS, TB), BF), pltpu.VMEM((D, TB2), BF), pltpu.VMEM((2, NB, FP, DS), BF), pltpu.VMEM((2, DS, KP), BF),
            DMA((6,)), DMA((2,)), DMA((2, 7)), DMA((2, 7)),
        ] + X_SEMS + FIRST_SEMS + SECOND_SEMS + FIRST_SEMS,
        compiler_params=params(1),
        cost_estimate=cost(120),
        name="first_exchange",
    )(xt, nw, w, idx, wd)


def up_kernel(split, h_ref, idx_ref, rt_hbm, wd_part, *refs):
    w_refs, refs = refs[:1 + split], refs[1 + split:]
    a_all, g_ref, wd_all, wv, slots, logits, a_buf, w_sem, rt_sem, local_sem = refs[:10]
    sems = refs[10:]
    step = pl.program_id(0)
    f = lax.axis_index("fsdp")
    mine = lambda owner: pl.ds(pl.multiple_of(owner * FP, 8), FP)
    ring = x_ring(lambda k: a_buf.at[k], lambda owner, k: a_all.at[k, :, mine(owner)], *sems[:2])
    second = second_rings(wd_all, False, sems[2:])

    def own_a(k):
        return pltpu.make_async_copy(a_buf.at[k], a_all.at[k, :, mine(f)], local_sem.at[k])

    def loads(g):
        out = [pltpu.make_async_copy(rt_hbm, wv.at[g, pl.ds(GROWS, E)], rt_sem.at[g])]
        for i in range(GE):
            at = 0
            for n, w in enumerate(w_refs):
                size = w.shape[1]
                out.append(pltpu.make_async_copy(w.at[g * GE + i], wv.at[g, pl.ds(i * RE + at, size)], w_sem.at[g, n, i]))
                at += size
        return out

    @pl.when(step == 0)
    def _():
        for g in range(STEPS):
            for c in loads(g):
                c.start()
        greet(x_neighbours() + yz_neighbours())
        start(second)

    slots[...] = jnp.zeros_like(slots)
    idx = jnp.concatenate([idx_ref[0], idx_ref[1]], axis=1)

    def group(g, carry):
        tick = step * STEPS + g

        @pl.when(step == 0)
        def _():
            for c in loads(g):
                c.wait()

        @pl.when(jnp.logical_and(step >= 1, g == 3))
        def _():
            for tb in range(2):
                ring.relay(2 * step - 2 + tb, tb == 1)

        for k in range(4):
            @pl.when(tick == 4 + 3 * k)
            def _(k=k):
                relay(second, k)

        res = jnp.dot(wv[g], h_ref[0], preferred_element_type=F32)
        logits[...] = res[GROWS:]
        for i in range(GE):
            at, parts = i * RE, []
            for n in (FA, FP - FA):
                parts.append(jax.nn.silu(res[at:at + n]) * res[at + n:at + 2 * n])
                at += 2 * n
            act = jnp.concatenate(parts, axis=0)
            for j in range(K):
                slots[j] = jnp.where(idx[j:j + 1] == g * GE + i, act, slots[j])
        return carry

    lax.fori_loop(0, STEPS, group, 0)
    for tb in range(2):
        a_buf[2 * step + tb] = slots[:, :, tb * TB:(tb + 1) * TB].astype(BF)
    eids = lax.broadcasted_iota(jnp.int32, (E, TB2), 0)
    chosen = idx[0:1] == eids
    for j in range(1, K):
        chosen = jnp.logical_or(chosen, idx[j:j + 1] == eids)
    lg = jnp.where(chosen, logits[...], -jnp.inf)
    ex = jnp.where(chosen, jnp.exp(lg - jnp.max(lg, axis=0, keepdims=True)), 0.0)
    gates = ex / jnp.sum(ex, axis=0, keepdims=True)
    for tb in range(2):
        g_ref[tb] = gates[:, tb * TB:(tb + 1) * TB]
    for tb in range(2):
        ring.start(2 * step + tb)
        own_a(2 * step + tb).start()

    @pl.when(step == 3)
    def _():
        for k in (6, 7):
            ring.relay(k, k % 2 == 1)
        for k in range(NB):
            ring.last(k)
        for k in range(NB):
            ring.from_partner(k)
            own_a(k).wait()
        ring.drain()
        finish(second)


def pair(*tail):
    return pl.BlockSpec((2,) + tail, lambda i: (i,) + (0,) * len(tail))


def whole(*dims):
    return pl.BlockSpec(dims, lambda i: (0,) * len(dims))


def up_proj(h, idx, rt, wd_part, ws):
    split = len(ws) - 1
    return pl.pallas_call(
        lambda *refs: up_kernel(split, *refs),
        grid=(STEPS,),
        out_shape=(shape((NB, K, NB * FP, TB)), shape((NB, E, TB), F32), shape((E, DS, KP))),
        in_specs=[pl.BlockSpec((1, D, TB2), lambda i: (i, 0, 0)), pair(K, TB), ANY, ANY] + [ANY] * len(ws),
        out_specs=(ANY, pair(E, TB), ANY),
        scratch_shapes=[
            pltpu.VMEM((STEPS, GROWS + E, D), BF),
            pltpu.VMEM((K, FP, TB2), F32),
            pltpu.VMEM((E, TB2), F32),
            pltpu.VMEM((NB, K, FP, TB), BF),
            DMA((STEPS, 2, GE)), DMA((STEPS,)), DMA((NB,)),
        ] + X_SEMS + SECOND_SEMS,
        input_output_aliases={3: 2},
        compiler_params=params(2 + split),
        cost_estimate=cost(70),
        name="up_proj",
    )(h, idx, rt, wd_part, *ws)


def down_block(a_ref, idx_ref, g_ref, wd_ref, acc, hook):
    idx = jnp.concatenate([idx_ref[0], idx_ref[1]], axis=1).astype(F32).astype(BF)
    acc[...] = jnp.zeros_like(acc)

    def group(g, carry):
        hook(g)
        for i in range(GE):
            e = g * GE + i
            ef = e.astype(F32).astype(BF)
            parts = []
            for tb in range(2):
                sel = jnp.zeros((NB * FP, TB), BF)
                for j in range(K):
                    row = idx[j:j + 1, tb * TB:(tb + 1) * TB]
                    sel = jnp.where(row == ef, a_ref[tb, j], sel)
                parts.append(sel)
            out = jnp.dot(wd_ref[e, :, :NB * FP], jnp.concatenate(parts, axis=1), preferred_element_type=F32)
            gate = jnp.concatenate([g_ref[0, pl.ds(e, 1)], g_ref[1, pl.ds(e, 1)]], axis=1)
            acc[...] += gate * out
        return carry

    lax.fori_loop(0, STEPS, group, 0)


def new_x(x, acc, tb):
    return (x.astype(F32) + acc[:, tb * TB:(tb + 1) * TB]).astype(BF)


def down_mid_kernel(
    a_ref, idx_ref, g_ref, x_ref, wd_ref, nw_ref, wd_next, x_all, h_all, wd_all, acc, o_buf, stage, h_stage, local_sem, norm_sem, *sems,
):
    step = pl.program_id(0)
    f = lax.axis_index("fsdp")
    ring = x_ring(lambda k: o_buf.at[k], lambda owner, k: x_all.at[owner, k], *sems[:2])
    d_first = first_rings(wd_next, wd_all, False, sems[2:])
    own_wd = pltpu.make_async_copy(wd_next, wd_all.at[lax.axis_index("ep")], local_sem.at[NB])

    def own_x(k):
        return pltpu.make_async_copy(o_buf.at[k], x_all.at[f, k], local_sem.at[k])

    @pl.when(step == 0)
    def _():
        greet(x_neighbours() + yz_neighbours())
        own_wd.start()
        start(d_first)

    def hook(g):
        @pl.when(jnp.logical_and(step >= 2, g == 2))
        def _():
            for tb in range(2):
                ring.relay(2 * step - 4 + tb, tb == 1)
            for k in range(2):
                @pl.when(step == 2 + k)
                def _(k=k):
                    relay(d_first, k)

    down_block(a_ref, idx_ref, g_ref, wd_ref, acc, hook)
    for tb in range(2):
        o_buf[2 * step + tb] = new_x(x_ref[tb, 0], acc, tb)
    for tb in range(2):
        ring.start(2 * step + tb)
        own_x(2 * step + tb).start()

    @pl.when(step == 3)
    def _():
        for i in range(STEPS):
            for k in (2 * i, 2 * i + 1):
                ring.last(k)
            for k in (2 * i, 2 * i + 1):
                ring.from_partner(k)
                own_x(k).wait()
            norm_block(x_all.at[:, pl.ds(2 * i, 2)], nw_ref, stage, h_stage, h_all.at[i], norm_sem, False)
            if i < 2:
                for k in (2 * i + 4, 2 * i + 5):
                    ring.relay(k, k % 2 == 1)
        ring.drain()
        own_wd.wait()
        finish(d_first)


def down_mid(a, idx, gates, x_all, wd, nw, wd_next):
    return pl.pallas_call(
        down_mid_kernel,
        grid=(STEPS,),
        out_shape=(shape((NB, NB, DS, TB)), shape((STEPS, D, TB2)), shape((E, DS, KP))),
        in_specs=[
            pair(K, NB * FP, TB), pair(K, TB), pair(E, TB),
            pl.BlockSpec((2, 1, DS, TB), lambda i: (i, lax.axis_index("fsdp"), 0, 0)),
            whole(E, DS, KP), whole(NB, DS, 128), whole(DS, KP),
        ],
        out_specs=[ANY] * 3,
        scratch_shapes=[
            pltpu.VMEM((DS, TB2), F32), pltpu.VMEM((NB, DS, TB), BF), pltpu.VMEM((NB, 2, DS, TB), BF), pltpu.VMEM((D, TB2), BF),
            DMA((NB + 1,)), DMA((2,)),
        ] + X_SEMS + FIRST_SEMS,
        compiler_params=params(4),
        cost_estimate=cost(80),
        name="down_mid",
    )(a, idx, gates, x_all, wd, nw, wd_next)


def down_last_kernel(a_ref, idx_ref, g_ref, x_ref, wd_ref, o_all, acc, o_buf, send_sem, recv_sem, local_sem):
    step = pl.program_id(0)
    f = lax.axis_index("fsdp")
    core = f % 2

    @pl.when(step == 0)
    def _():
        greet([{"fsdp": fsdp_at(s, o)} for s, o in PEERS])

    down_block(a_ref, idx_ref, g_ref, wd_ref, acc, lambda g: None)
    for tb in range(2):
        o_buf[step, tb] = new_x(x_ref[0, tb], acc, tb)

    def send(s, o):
        return remote(o_buf.at[(s + 3) % 4, 1 - core if o else core], o_all.at[f], send_sem.at[s, o], recv_sem.at[s, o], {"fsdp": fsdp_at(s, o)})

    for s in range(1, 4):
        @pl.when(step == s - 1)
        def _(s=s):
            send(s, 0).start()
            send(s, 1).start()

    @pl.when(step == 3)
    def _():
        send(0, 1).start()
        mine = pltpu.make_async_copy(o_buf.at[3, core], o_all.at[f], local_sem)
        mine.start()
        for s, o in PEERS:
            source = fsdp_at((4 - s) % 4, o)
            remote(o_buf.at[0, 0], o_all.at[source], send_sem.at[s, o], recv_sem.at[s, o], {"fsdp": source}).wait_recv()
        for s, o in PEERS:
            send(s, o).wait_send()
        mine.wait()


def down_last(a, idx, gates, x_all, wd):
    block = lambda i: lax.rem(lax.axis_index("fsdp") // 2 + 1 + i, 4)

    def turned(*tail):
        return pl.BlockSpec((2,) + tail, lambda i: (block(i),) + (0,) * len(tail))

    return pl.pallas_call(
        down_last_kernel,
        grid=(STEPS,),
        out_shape=shape((NB, DS, TB)),
        in_specs=[
            turned(K, NB * FP, TB), turned(K, TB), turned(E, TB),
            pl.BlockSpec((1, 2, DS, TB), lambda i: (lax.axis_index("fsdp"), block(i), 0, 0)),
            whole(E, DS, KP),
        ],
        out_specs=ANY,
        scratch_shapes=[pltpu.VMEM((DS, TB2), F32), pltpu.VMEM((STEPS, 2, DS, TB), BF), DMA((4, 2)), DMA((4, 2)), DMA],
        compiler_params=params(5),
        cost_estimate=cost(45),
        name="down_last",
    )(a, idx, gates, x_all, wd)


def solution(mesh):
    tok_spec = P(("rep", "ep", "fsdp"), None)
    idx_spec = P(None, ("rep", "ep", "fsdp"), None)
    in_specs = (tok_spec, P(None, None), P(None, None, None), P(None, "ep", None, "fsdp"), P(None, "ep", None, "fsdp"), P(None, "ep", "fsdp", None), idx_spec)

    def local_program(x, norm_w, router_w, w_gate, w_up, w_down, expert_idx):
        pad = jnp.zeros((FP - F, D), BF)
        nws = [jnp.broadcast_to(n.reshape(NB, DS, 1), (NB, DS, 128)) for n in norm_w]
        routers = [r.T for r in router_w]

        def pack(gate, up):
            gate, up = gate.T, up.T
            return [gate[:FA], up[:FA]], [gate[FA:], pad, up[FA:], pad]

        part_a, part_b = [jnp.concatenate(p, axis=0) for p in pack(w_gate[0, 0], w_up[0, 0])]
        w_a = lax.all_gather(part_a, "ep", axis=0, tiled=False)
        gate1, up1, _ = lax.optimization_barrier((w_gate, w_up, part_a))
        one, two = pack(gate1[1, 0], up1[1, 0])
        rows = jnp.concatenate(one + two, axis=0)
        wd = jnp.pad(w_down[:, 0], ((0, 0), (0, FP - F), (0, 0))).reshape(2, FP, NB, DS).swapaxes(1, 2)
        xt = x.T.reshape(NB, DS, TB)
        xt, idx, wd, part_b, rows = lax.optimization_barrier((xt, jnp.swapaxes(expert_idx, 1, 2), wd, part_b, rows))
        x_all, h, w_b, idx, wd_part, wd_next = first_exchange(xt, nws[0], part_b, idx, wd)
        rows, _ = lax.optimization_barrier((rows, idx))
        w_next = lax.all_gather(rows, "ep", axis=0, tiled=False)
        a, gates, wd_all = up_proj(h, idx[:, 0], routers[0], wd_part, (w_a, w_b))
        x_all, h, wd_part = down_mid(a, idx[:, 0], gates, x_all, wd_all, nws[1], wd_next)
        a, gates, wd_all = up_proj(h, idx[:, 1], routers[1], wd_part, (w_next,))
        return down_last(a, idx[:, 1], gates, x_all, wd_all).reshape(D, TB).T

    return jax.shard_map(local_program, mesh=mesh, in_specs=in_specs, out_specs=tok_spec, check_vma=False)
```

```python
import jax
import jax.numpy as jnp
from jax import lax
from jax.experimental import pallas as pl
from jax.experimental.pallas import tpu as pltpu
from jax.sharding import PartitionSpec as P

NORM_EPS = 1e-5
TB = 256
TB2 = 512
NB = 8
D = 4096
DS = 512
F = 86
FP = 88
FA = 48
RA = 96
RB = 80
RE = 176
KP = 768
E = 16
K = 4
STEPS = 4
GE = 4
GROWS = GE * RE
BF = jnp.bfloat16
F32 = jnp.float32
MESH = pl.DeviceIdType.MESH
DMA = pltpu.SemaphoreType.DMA
ANY = pl.BlockSpec(memory_space=pl.ANY)
IN_VMEM = pl.BlockSpec(memory_space=pltpu.VMEM)
PEERS = [(s, o) for s in range(4) for o in range(2) if s + o]


def shape(dims, dtype=BF):
    return jax.ShapeDtypeStruct(dims, dtype)


def params(collective_id):
    return pltpu.CompilerParams(vmem_limit_bytes=67_000_000, collective_id=collective_id, has_side_effects=True)


def cost(micros):
    return pl.CostEstimate(flops=micros * 1_000_000_000, bytes_accessed=10_000_000, transcendentals=0)


def remote(src, dst, send_sem, recv_sem, device):
    return pltpu.make_async_remote_copy(src_ref=src, dst_ref=dst, send_sem=send_sem, recv_sem=recv_sem, device_id=device, device_id_type=MESH)


def fsdp_at(step, other=0):
    f = lax.axis_index("fsdp")
    core = f % 2
    return lax.rem(f // 2 + step, 4) * 2 + (1 - core if other else core)


def greet(devices):
    barrier = pltpu.get_barrier_semaphore()
    for d in devices:
        pl.semaphore_signal(barrier, inc=1, device_id=d, device_id_type=MESH)
    pl.semaphore_wait(barrier, len(devices))


class Ring:
    def __init__(self, pos, dev, own, place, chunks, send_sem, recv_sem, partner=None):
        self.pos, self.dev, self.own, self.place, self.chunks = pos, dev, own, place, chunks
        self.send_sem, self.recv_sem, self.partner = send_sem, recv_sem, partner
        self.right, self.left, self.far = [lax.rem(pos + s, 4) for s in (1, 3, 2)]

    def copy(self, kind, k, src, dst, device):
        return remote(src, dst, self.send_sem.at[kind, k], self.recv_sem.at[kind, k], device)

    def own_copies(self, k):
        mine = self.place(self.pos, k)
        out = [self.copy(0, k, self.own(k), mine, self.dev(self.right)), self.copy(1, k, self.own(k), mine, self.dev(self.left))]
        if self.partner is not None:
            out.append(self.copy(3, k, self.own(k), mine, self.partner))
        return out

    def onward(self, k, odd):
        source, target = (self.right, self.left) if odd else (self.left, self.right)
        ref = self.place(source, k)
        return self.copy(2, k, ref, ref, self.dev(target))

    def across(self, kind, k):
        ref = self.place({4: self.left, 5: self.right, 6: self.far}[kind], k)
        return self.copy(kind, k, ref, ref, self.partner)

    def arrived(self, kind, k, pos, *other):
        ref = self.place(pos, k, *other)
        self.copy(kind, k, ref, ref, self.dev(self.right)).wait_recv()

    def start(self, k):
        for c in self.own_copies(k):
            c.start()

    def relay(self, k, odd):
        for kind, pos, onward in ((0, self.left, not odd), (1, self.right, odd)):
            self.arrived(kind, k, pos)
            if onward:
                self.onward(k, odd).start()
            if self.partner is not None:
                self.across(4 + kind, k).start()

    def last(self, k):
        self.arrived(2, k, self.far)
        if self.partner is not None:
            self.across(6, k).start()

    def from_partner(self, k):
        for kind, pos in ((3, self.pos), (4, self.left), (5, self.right), (6, self.far)):
            self.arrived(kind, k, pos, 1)

    def drain(self):
        for k in range(self.chunks):
            for c in self.own_copies(k):
                c.wait_send()
            self.onward(k, k % 2 == 1).wait_send()
            if self.partner is not None:
                for kind in (4, 5, 6):
                    self.across(kind, k).wait_send()


def x_ring(own, place, send_sem, recv_sem):
    f = lax.axis_index("fsdp")
    core = f % 2

    def where(p, k, other=0):
        return place(p * 2 + (1 - core if other else core), k)

    return Ring(f // 2, lambda p: {"fsdp": p * 2 + core}, own, where, NB, send_sem, recv_sem, {"fsdp": fsdp_at(0, 1)})


X_SEMS = [DMA((7, NB)), DMA((7, NB))]
FIRST_SEMS = [DMA((2, 3, 2)), DMA((2, 3, 2))]
SECOND_SEMS = [DMA((2, 3, 4)), DMA((2, 3, 4))]


def x_neighbours():
    return [{"fsdp": fsdp_at(1)}, {"fsdp": fsdp_at(3)}, {"fsdp": fsdp_at(0, 1)}]


def yz():
    e = lax.axis_index("ep")
    z, y = e // 4, e % 4
    return z, y, (lambda p: {"ep": p * 4 + y}), (lambda p: {"ep": z * 4 + p})


def yz_neighbours():
    z, y, on_z, on_y = yz()
    return [f(lax.rem(p + s, 4)) for f, p in ((on_z, z), (on_y, y)) for s in (1, 3)]


def cut(ref, lanes, half, chunk=None):
    size = ref.shape[1 if lanes else 0] // 2
    span = pl.ds(half * size, size) if chunk is None else pl.ds(half * size + chunk * (size // 2), size // 2)
    return ref.at[:, span] if lanes else ref.at[span]


def first_rings(own, full, lanes, sems):
    z, y, on_z, on_y = yz()
    send, recv = sems
    return [
        Ring(y, on_y, lambda k: cut(own, lanes, 0, k), lambda p, k: cut(full.at[z * 4 + p], lanes, 0, k), 2, send.at[0], recv.at[0]),
        Ring(z, on_z, lambda k: cut(own, lanes, 1, k), lambda p, k: cut(full.at[p * 4 + y], lanes, 1, k), 2, send.at[1], recv.at[1]),
    ]


def second_rings(full, lanes, sems):
    z, y, on_z, on_y = yz()
    send, recv = sems
    by_z = lambda p, k: cut(full.at[p * 4 + k], lanes, 0)
    by_y = lambda p, k: cut(full.at[k * 4 + p], lanes, 1)
    return [
        Ring(z, on_z, lambda k: by_z(z, k), by_z, 4, send.at[0], recv.at[0]),
        Ring(y, on_y, lambda k: by_y(y, k), by_y, 4, send.at[1], recv.at[1]),
    ]


def start(rings):
    for k in range(rings[0].chunks):
        for r in rings:
            r.start(k)


def relay(rings, k):
    for r in rings:
        r.relay(k, k % 2 == 1)


def finish(rings):
    for r in rings:
        for k in range(r.chunks):
            r.last(k)
        r.drain()


def norm_block(view, nw_ref, stage, h_stage, h_out, sems, tok_major):
    load = pltpu.make_async_copy(view, stage, sems.at[0])
    load.start()
    load.wait()
    for tb in range(2):
        def rows(c, tb=tb):
            return (stage[tb, c] if tok_major else stage[c, tb]).astype(F32)

        def ssq_body(c, acc):
            xf = rows(c)
            return acc + jnp.sum(xf * xf, axis=0, keepdims=True)

        ssq = lax.fori_loop(0, NB, ssq_body, jnp.zeros((1, TB), F32))
        rstd = lax.rsqrt(ssq * (1.0 / D) + NORM_EPS)

        def h_body(c, carry, tb=tb, rstd=rstd):
            nw = nw_ref[c]
            nw2 = jnp.concatenate([nw, nw], axis=1)
            h_stage[pl.ds(pl.multiple_of(c * DS, DS), DS), tb * TB:(tb + 1) * TB] = (rows(c) * rstd * nw2).astype(BF)
            return carry

        lax.fori_loop(0, NB, h_body, 0)
    store = pltpu.make_async_copy(h_stage, h_out, sems.at[1])
    store.start()
    store.wait()


def first_kernel(
    x_ref, nw_ref, w_ref, idx_ref, wd_ref, x_all, h_all, w_all, idx_all, wd_all, wd_next,
    stage, h_stage, wd_in, wd_out, local_sem, norm_sem, small_send, small_recv, *sems,
):
    f, e = lax.axis_index("fsdp"), lax.axis_index("ep")
    greet([{"fsdp": fsdp_at(s, o)} for s, o in PEERS] + yz_neighbours())
    ring = x_ring(lambda k: x_ref.at[k], lambda owner, k: x_all.at[owner, k], *sems[:2])
    w_first = first_rings(w_ref, w_all, True, sems[2:4])
    w_second = second_rings(w_all, True, sems[4:6])
    d_first = first_rings(wd_out.at[0], wd_all, False, sems[6:])
    own = [pltpu.make_async_copy(src, dst, local_sem.at[i])
           for i, (src, dst) in enumerate((
               (w_ref, w_all.at[e]), (x_ref, x_all.at[f]), (wd_ref.at[:, f], wd_in.at[:, f]), (idx_ref, idx_all.at[f])))]
    after = [pltpu.make_async_copy(wd_out.at[0], wd_all.at[e], local_sem.at[4]), pltpu.make_async_copy(wd_out.at[1], wd_next, local_sem.at[5])]
    small = []
    for p, (s, o) in enumerate(PEERS):
        peer = fsdp_at(s, o)
        small.append(remote(wd_ref.at[:, peer], wd_in.at[:, f], small_send.at[0, p], small_recv.at[0, p], {"fsdp": peer}))
        small.append(remote(idx_ref, idx_all.at[f], small_send.at[1, p], small_recv.at[1, p], {"fsdp": peer}))
    start(w_first)
    for c in small + own:
        c.start()
    for k in range(NB):
        ring.start(k)
    for p, (s, o) in enumerate(PEERS):
        source = fsdp_at((4 - s) % 4, o)
        remote(wd_ref.at[:, 0], wd_in.at[:, source], small_send.at[0, p], small_recv.at[0, p], {"fsdp": source}).wait_recv()
        remote(idx_ref, idx_all.at[source], small_send.at[1, p], small_recv.at[1, p], {"fsdp": source}).wait_recv()
    for c in own[2:]:
        c.wait()
    for l in range(2):
        wd_out[l, :, :NB * FP] = jnp.swapaxes(wd_in[l].reshape(NB * FP, DS), 0, 1)
        wd_out[l, :, NB * FP:] = jnp.zeros((DS, KP - NB * FP), BF)
    relay(w_first, 0)
    for k in range(NB):
        ring.relay(k, k % 2 == 1)
        if k == 0:
            relay(w_first, 1)
            for c in after:
                c.start()
            start(d_first)
        if k == 3:
            finish(w_first)
            own[0].wait()
            start(w_second)
        if k in (5, 6):
            relay(d_first, k - 5)
    for k in range(NB):
        ring.last(k)
        if k in (0, 4):
            relay(w_second, k // 4)
    for k in range(NB):
        ring.from_partner(k)
    own[1].wait()
    for i in range(STEPS):
        if i < 2:
            relay(w_second, i + 2)
        norm_block(x_all.at[pl.ds(2 * i, 2)], nw_ref, stage, h_stage, h_all.at[i], norm_sem, True)
    finish(d_first)
    for c in after:
        c.wait()
    finish(w_second)
    ring.drain()
    for c in small:
        c.wait_send()


def first_exchange(xt, nw, w, idx, wd):
    return pl.pallas_call(
        first_kernel,
        out_shape=(
            shape((NB, NB, DS, TB)), shape((STEPS, D, TB2)), shape((E,) + w.shape), shape((NB,) + idx.shape, jnp.int32),
            shape((E, DS, KP)), shape((DS, KP))),
        in_specs=[IN_VMEM] * 5,
        out_specs=[ANY] * 6,
        scratch_shapes=[
            pltpu.VMEM((2, NB, DS, TB), BF), pltpu.VMEM((D, TB2), BF), pltpu.VMEM((2, NB, FP, DS), BF), pltpu.VMEM((2, DS, KP), BF),
            DMA((6,)), DMA((2,)), DMA((2, 7)), DMA((2, 7)),
        ] + X_SEMS + FIRST_SEMS + SECOND_SEMS + FIRST_SEMS,
        compiler_params=params(1),
        cost_estimate=cost(120),
        name="first_exchange",
    )(xt, nw, w, idx, wd)


def weight_loads(g, w_refs, rt_hbm, wv, w_sem, rt_sem):
    out = [pltpu.make_async_copy(rt_hbm, wv.at[g, pl.ds(GROWS, E)], rt_sem.at[g])]
    for i in range(GE):
        at = 0
        for n, w in enumerate(w_refs):
            size = w.shape[1]
            out.append(pltpu.make_async_copy(w.at[g * GE + i], wv.at[g, pl.ds(i * RE + at, size)], w_sem.at[g, n, i]))
            at += size
    return out


def up_block(h_ref, idx, wv, slots, logits, split, hook):
    slots[...] = jnp.zeros_like(slots)

    def group(g, carry):
        hook(g)
        res = jnp.dot(wv[g], h_ref[0], preferred_element_type=F32)
        logits[...] = res[GROWS:]
        for i in range(GE):
            at, parts = i * RE, []
            for n in (FA, FP - FA) if split else (FP,):
                parts.append(jax.nn.silu(res[at:at + n]) * res[at + n:at + 2 * n])
                at += 2 * n
            act = jnp.concatenate(parts, axis=0) if split else parts[0]
            for j in range(K):
                slots[j] = jnp.where(idx[j:j + 1] == g * GE + i, act, slots[j])
        return carry

    lax.fori_loop(0, STEPS, group, 0)
    eids = lax.broadcasted_iota(jnp.int32, (E, TB2), 0)
    chosen = idx[0:1] == eids
    for j in range(1, K):
        chosen = jnp.logical_or(chosen, idx[j:j + 1] == eids)
    lg = jnp.where(chosen, logits[...], -jnp.inf)
    ex = jnp.where(chosen, jnp.exp(lg - jnp.max(lg, axis=0, keepdims=True)), 0.0)
    return ex / jnp.sum(ex, axis=0, keepdims=True)


def both(ref):
    return jnp.concatenate([ref[0], ref[1]], axis=1)


def when_all(*conditions):
    out = conditions[0]
    for c in conditions[1:]:
        out = jnp.logical_and(out, c)
    return pl.when(out)


def up_kernel(h_ref, idx_ref, rt_hbm, wd_part, w_a, w_b, a_all, g_ref, wd_all, wv, slots, logits, a_buf, w_sem, rt_sem, local_sem, *sems):
    step = pl.program_id(0)
    f = lax.axis_index("fsdp")
    mine = lambda owner: pl.ds(pl.multiple_of(owner * FP, 8), FP)
    ring = x_ring(lambda k: a_buf.at[k], lambda owner, k: a_all.at[k, :, mine(owner)], *sems[:2])
    second = second_rings(wd_all, False, sems[2:])
    loads = lambda g: weight_loads(g, (w_a, w_b), rt_hbm, wv, w_sem, rt_sem)

    def own_a(k):
        return pltpu.make_async_copy(a_buf.at[k], a_all.at[k, :, mine(f)], local_sem.at[k])

    @pl.when(step == 0)
    def _():
        for g in range(STEPS):
            for c in loads(g):
                c.start()
        greet(x_neighbours() + yz_neighbours())
        start(second)

    def hook(g):
        @pl.when(step == 0)
        def _():
            for c in loads(g):
                c.wait()

        @when_all(step >= 1, g == 3)
        def _():
            for tb in range(2):
                ring.relay(2 * step - 2 + tb, tb == 1)

        for k in range(4):
            @pl.when(step * STEPS + g == 4 + 3 * k)
            def _(k=k):
                relay(second, k)

    gates = up_block(h_ref, both(idx_ref), wv, slots, logits, True, hook)
    for tb in range(2):
        a_buf[2 * step + tb] = slots[:, :, tb * TB:(tb + 1) * TB].astype(BF)
        g_ref[tb] = gates[:, tb * TB:(tb + 1) * TB]
    for tb in range(2):
        ring.start(2 * step + tb)
        own_a(2 * step + tb).start()

    @pl.when(step == 3)
    def _():
        for k in (6, 7):
            ring.relay(k, k % 2 == 1)
        for k in range(NB):
            ring.last(k)
        for k in range(NB):
            ring.from_partner(k)
            own_a(k).wait()
        ring.drain()
        finish(second)


def pair(*tail):
    return pl.BlockSpec((2,) + tail, lambda i: (i,) + (0,) * len(tail))


def whole(*dims):
    return pl.BlockSpec(dims, lambda i: (0,) * len(dims))


UP_SCRATCH = [
    pltpu.VMEM((STEPS, GROWS + E, D), BF),
    pltpu.VMEM((K, FP, TB2), F32),
    pltpu.VMEM((E, TB2), F32),
    pltpu.VMEM((NB, K, FP, TB), BF),
    DMA((STEPS, 2, GE)), DMA((STEPS,)), DMA((NB,)),
]


def up_proj(h, idx, rt, wd_part, w_a, w_b):
    return pl.pallas_call(
        up_kernel,
        grid=(STEPS,),
        out_shape=(shape((NB, K, NB * FP, TB)), shape((NB, E, TB), F32), shape((E, DS, KP))),
        in_specs=[pl.BlockSpec((1, D, TB2), lambda i: (i, 0, 0)), pair(K, TB)] + [ANY] * 4,
        out_specs=(ANY, pair(E, TB), ANY),
        scratch_shapes=UP_SCRATCH + X_SEMS + SECOND_SEMS,
        input_output_aliases={3: 2},
        compiler_params=params(2),
        cost_estimate=cost(70),
        name="up_proj",
    )(h, idx, rt, wd_part, w_a, w_b)


def down_block(a_ref, idx_ref, g_ref, wd_ref, acc, hook):
    idx = both(idx_ref).astype(F32).astype(BF)
    acc[...] = jnp.zeros_like(acc)

    def group(g, carry):
        hook(g)
        for i in range(GE):
            e = g * GE + i
            ef = e.astype(F32).astype(BF)
            parts = []
            for tb in range(2):
                sel = jnp.zeros((NB * FP, TB), BF)
                for j in range(K):
                    row = idx[j:j + 1, tb * TB:(tb + 1) * TB]
                    sel = jnp.where(row == ef, a_ref[tb, j], sel)
                parts.append(sel)
            out = jnp.dot(wd_ref[e, :, :NB * FP], jnp.concatenate(parts, axis=1), preferred_element_type=F32)
            gate = jnp.concatenate([g_ref[0, pl.ds(e, 1)], g_ref[1, pl.ds(e, 1)]], axis=1)
            acc[...] += gate * out
        return carry

    lax.fori_loop(0, STEPS, group, 0)


def new_x(x, acc, tb):
    return (x.astype(F32) + acc[:, tb * TB:(tb + 1) * TB]).astype(BF)


def down_mid_kernel(
    a_ref, idx_ref, g_ref, x_ref, wd_ref, nw_ref, wd_next, x_all, h_all, wd_all, acc, o_buf, stage, h_stage, local_sem, norm_sem, *sems,
):
    step = pl.program_id(0)
    f = lax.axis_index("fsdp")
    ring = x_ring(lambda k: o_buf.at[k], lambda owner, k: x_all.at[owner, k], *sems[:2])
    d_first = first_rings(wd_next, wd_all, False, sems[2:])
    own_wd = pltpu.make_async_copy(wd_next, wd_all.at[lax.axis_index("ep")], local_sem.at[NB])

    def own_x(k):
        return pltpu.make_async_copy(o_buf.at[k], x_all.at[f, k], local_sem.at[k])

    @pl.when(step == 0)
    def _():
        greet(x_neighbours() + yz_neighbours())
        own_wd.start()
        start(d_first)

    def hook(g):
        @pl.when(jnp.logical_and(step >= 2, g == 2))
        def _():
            for tb in range(2):
                ring.relay(2 * step - 4 + tb, tb == 1)
            for k in range(2):
                @pl.when(step == 2 + k)
                def _(k=k):
                    relay(d_first, k)

    down_block(a_ref, idx_ref, g_ref, wd_ref, acc, hook)
    for tb in range(2):
        o_buf[2 * step + tb] = new_x(x_ref[tb, 0], acc, tb)
    for tb in range(2):
        ring.start(2 * step + tb)
        own_x(2 * step + tb).start()

    @pl.when(step == 3)
    def _():
        for i in range(STEPS):
            for k in (2 * i, 2 * i + 1):
                ring.last(k)
            for k in (2 * i, 2 * i + 1):
                ring.from_partner(k)
                own_x(k).wait()
            norm_block(x_all.at[:, pl.ds(2 * i, 2)], nw_ref, stage, h_stage, h_all.at[i], norm_sem, False)
            if i < 2:
                for k in (2 * i + 4, 2 * i + 5):
                    ring.relay(k, k % 2 == 1)
        ring.drain()
        own_wd.wait()
        finish(d_first)


def down_mid(a, idx, gates, x_all, wd, nw, wd_next):
    return pl.pallas_call(
        down_mid_kernel,
        grid=(STEPS,),
        out_shape=(shape((NB, NB, DS, TB)), shape((STEPS, D, TB2)), shape((E, DS, KP))),
        in_specs=[
            pair(K, NB * FP, TB), pair(K, TB), pair(E, TB),
            pl.BlockSpec((2, 1, DS, TB), lambda i: (i, lax.axis_index("fsdp"), 0, 0)),
            whole(E, DS, KP), whole(NB, DS, 128), whole(DS, KP),
        ],
        out_specs=[ANY] * 3,
        scratch_shapes=[
            pltpu.VMEM((DS, TB2), F32), pltpu.VMEM((NB, DS, TB), BF), pltpu.VMEM((NB, 2, DS, TB), BF), pltpu.VMEM((D, TB2), BF),
            DMA((NB + 1,)), DMA((2,)),
        ] + X_SEMS + FIRST_SEMS,
        compiler_params=params(4),
        cost_estimate=cost(80),
        name="down_mid",
    )(a, idx, gates, x_all, wd, nw, wd_next)


CODES = (17, 74, 191, 228)


def turn(n):
    ring = lax.axis_index("fsdp") // 2
    place = (1 + 3 * (ring % 2)) * (1 + 15 * (ring // 2))
    out = 0
    for i in range(STEPS):
        out = out + jnp.where(n == i, (CODES[i] // place) % 4, 0)
    return out


def last_kernel(
    h_ref, idx_ref, rt_hbm, wd_part, w, x_ref, o_all, a_all, wd_all, wv, slots, logits, a_buf, w_sem, rt_sem, local_sem,
    g_v, wd_v, a_v, acc, o_buf, wd_sem, a_sem, out_send, out_recv, *sems,
):
    step = pl.program_id(0)
    f = lax.axis_index("fsdp")
    core = f % 2
    mine = lambda owner: pl.ds(pl.multiple_of(owner * FP, 8), FP)
    ring = x_ring(lambda k: a_buf.at[k], lambda owner, k: a_all.at[k, :, mine(owner)], *sems[:2])
    second = second_rings(wd_all, False, sems[2:])
    loads = lambda g: weight_loads(g, (w,), rt_hbm, wv, w_sem, rt_sem)

    def own_a(k):
        return pltpu.make_async_copy(a_buf.at[k], a_all.at[k, :, mine(f)], local_sem.at[k])

    def wd_load(g):
        return pltpu.make_async_copy(wd_all.at[pl.ds(g * GE, GE)], wd_v.at[pl.ds(g * GE, GE)], wd_sem.at[g])

    def a_load(n):
        return pltpu.make_async_copy(a_all.at[pl.ds(2 * turn(n), 2)], a_v.at[n % 2], a_sem.at[n % 2])

    def complete(chunks):
        for k in chunks:
            ring.from_partner(k)
            own_a(k).wait()

    @pl.when(step == 0)
    def _():
        for g in range(STEPS):
            for c in loads(g):
                c.start()
        greet([{"fsdp": fsdp_at(s, o)} for s, o in PEERS] + yz_neighbours())
        start(second)

    def up_hook(g):
        @pl.when(step == 0)
        def _():
            for c in loads(g):
                c.wait()

        @when_all(step >= 1, g == 3)
        def _():
            for tb in range(2):
                ring.relay(2 * step - 2 + tb, tb == 1)

        for k in range(4):
            @pl.when(step * STEPS + g == 4 + 3 * k)
            def _(k=k):
                relay(second, k)

        @when_all(step == 3, g == 1)
        def _():
            for k in range(4):
                ring.last(k)

        @when_all(step == 3, g == 2)
        def _():
            complete(range(4))
            a_load(0).start()

    @pl.when(step < STEPS)
    def _():
        gates = up_block(h_ref, both(idx_ref.at[pl.ds(2 * step, 2)]), wv, slots, logits, False, up_hook)
        for tb in range(2):
            a_buf[2 * step + tb] = slots[:, :, tb * TB:(tb + 1) * TB].astype(BF)
            g_v[2 * step + tb] = gates[:, tb * TB:(tb + 1) * TB]
        for tb in range(2):
            ring.start(2 * step + tb)
            own_a(2 * step + tb).start()

    n = step - STEPS

    @pl.when(n == 0)
    def _():
        finish(second)
        for g in range(STEPS):
            wd_load(g).start()

    def down_hook(g):
        @pl.when(n == 0)
        def _():
            wd_load(g).wait()

        @when_all(n == 0, g == 1)
        def _():
            for k in (4, 5):
                ring.last(k)

        @when_all(n == 0, g == 2)
        def _():
            complete((4, 5))
            a_load(1).start()

        @when_all(n == 1, g == 0)
        def _():
            for k in (6, 7):
                ring.relay(k, k % 2 == 1)

        @when_all(n == 1, g == 3)
        def _():
            for k in (6, 7):
                ring.last(k)

        @when_all(n == 2, g == 0)
        def _():
            a_load(3).start()

    def send(i, other):
        return remote(
            o_buf.at[i, 1 - core if other else core], o_all.at[f], out_send.at[i, other], out_recv.at[f],
            {"fsdp": 2 * turn(i) + (1 - core if other else core)})

    @pl.when(n >= 0)
    def _():
        now = 2 * turn(n)
        a_load(n).wait()
        down_block(a_v.at[n % 2], idx_ref.at[pl.ds(now, 2)], g_v.at[pl.ds(now, 2)], wd_v, acc, down_hook)
        for tb in range(2):
            o_buf[n, tb] = new_x(x_ref[0, now + tb], acc, tb)
        send(n, 1).start()

        @pl.when(n < 3)
        def _():
            send(n, 0).start()

        @pl.when(n == 1)
        def _():
            complete((6, 7))
            a_load(2).start()

    @pl.when(n == 3)
    def _():
        own = pltpu.make_async_copy(o_buf.at[3, core], o_all.at[f], a_sem.at[0])
        own.start()
        ring.drain()
        for s, o in PEERS:
            source = fsdp_at(s, o)
            remote(o_buf.at[0, 0], o_all.at[source], out_send.at[0, 0], out_recv.at[source], {"fsdp": source}).wait_recv()
        for i in range(STEPS):
            send(i, 1).wait_send()
            if i < 3:
                send(i, 0).wait_send()
        own.wait()


def last_layer(h, idx, rt, wd_part, w, x_all):
    return pl.pallas_call(
        last_kernel,
        grid=(2 * STEPS,),
        out_shape=(shape((NB, DS, TB)), shape((NB, K, NB * FP, TB)), shape((E, DS, KP))),
        in_specs=[
            pl.BlockSpec((1, D, TB2), lambda i: (jnp.minimum(i, STEPS - 1), 0, 0)), whole(NB, K, TB), ANY, ANY, ANY,
            pl.BlockSpec((1, NB, DS, TB), lambda i: (lax.axis_index("fsdp"), 0, 0, 0), pipeline_mode=pl.Buffered(1)),
        ],
        out_specs=[ANY] * 3,
        scratch_shapes=UP_SCRATCH + [
            pltpu.VMEM((NB, E, TB), F32), pltpu.VMEM((E, DS, KP), BF), pltpu.VMEM((2, 2, K, NB * FP, TB), BF),
            pltpu.VMEM((DS, TB2), F32), pltpu.VMEM((STEPS, 2, DS, TB), BF),
            DMA((STEPS,)), DMA((2,)), DMA((4, 2)), DMA((NB,)),
        ] + X_SEMS + SECOND_SEMS,
        input_output_aliases={3: 2},
        compiler_params=params(3),
        cost_estimate=cost(110),
        name="last_layer",
    )(h, idx, rt, wd_part, w, x_all)


def solution(mesh):
    tok_spec = P(("rep", "ep", "fsdp"), None)
    idx_spec = P(None, ("rep", "ep", "fsdp"), None)
    in_specs = (tok_spec, P(None, None), P(None, None, None), P(None, "ep", None, "fsdp"), P(None, "ep", None, "fsdp"), P(None, "ep", "fsdp", None), idx_spec)

    def local_program(x, norm_w, router_w, w_gate, w_up, w_down, expert_idx):
        pad = jnp.zeros((FP - F, D), BF)
        nws = [jnp.broadcast_to(n.reshape(NB, DS, 1), (NB, DS, 128)) for n in norm_w]
        routers = [r.T for r in router_w]

        def pack(gate, up):
            gate, up = gate.T, up.T
            return [gate[:FA], up[:FA]], [gate[FA:], pad, up[FA:], pad]

        part_a, part_b = [jnp.concatenate(p, axis=0) for p in pack(w_gate[0, 0], w_up[0, 0])]
        w_a = lax.all_gather(part_a, "ep", axis=0, tiled=False)
        gate1, up1, _ = lax.optimization_barrier((w_gate, w_up, part_a))
        rows = jnp.concatenate([gate1[1, 0].T, pad, up1[1, 0].T, pad], axis=0)
        wd = jnp.pad(w_down[:, 0], ((0, 0), (0, FP - F), (0, 0))).reshape(2, FP, NB, DS).swapaxes(1, 2)
        xt = x.T.reshape(NB, DS, TB)
        xt, idx, wd, part_b, rows = lax.optimization_barrier((xt, jnp.swapaxes(expert_idx, 1, 2), wd, part_b, rows))
        x_all, h, w_b, idx, wd_part, wd_next = first_exchange(xt, nws[0], part_b, idx, wd)
        rows, _ = lax.optimization_barrier((rows, idx))
        w_next = lax.all_gather(rows, "ep", axis=0, tiled=False)
        a, gates, wd_all = up_proj(h, idx[:, 0], routers[0], wd_part, w_a, w_b)
        x_all, h, wd_part = down_mid(a, idx[:, 0], gates, x_all, wd_all, nws[1], wd_next)
        return last_layer(h, idx[:, 1], routers[1], wd_part, w_next, x_all)[0].reshape(D, TB).T

    return jax.shard_map(local_program, mesh=mesh, in_specs=in_specs, out_specs=tok_spec, check_vma=False)
```

```python
import jax
import jax.numpy as jnp
from jax import lax
from jax.experimental import pallas as pl
from jax.experimental.pallas import tpu as pltpu
from jax.sharding import PartitionSpec as P

NORM_EPS = 1e-5
TB = 256
TB2 = 512
NB = 8
D = 4096
DS = 512
F = 86
FP = 88
FA = 48
RE = 176
KP = 768
E = 16
K = 4
STEPS = 4
GE = 4
GROWS = GE * RE
BF = jnp.bfloat16
F32 = jnp.float32
MESH = pl.DeviceIdType.MESH
DMA = pltpu.SemaphoreType.DMA
ANY = pl.BlockSpec(memory_space=pl.ANY)
IN_VMEM = pl.BlockSpec(memory_space=pltpu.VMEM)
LATE = (6, 7)
MIDDLE = (4, 5)
PEERS = [(s, o) for s in range(4) for o in range(2) if s + o]


def shape(dims, dtype=BF):
    return jax.ShapeDtypeStruct(dims, dtype)


def params(collective_id):
    return pltpu.CompilerParams(vmem_limit_bytes=67_000_000, collective_id=collective_id, has_side_effects=True)


def cost(micros):
    return pl.CostEstimate(flops=micros * 1_000_000_000, bytes_accessed=10_000_000, transcendentals=0)


def remote(src, dst, send_sem, recv_sem, device):
    return pltpu.make_async_remote_copy(src_ref=src, dst_ref=dst, send_sem=send_sem, recv_sem=recv_sem, device_id=device, device_id_type=MESH)


def fsdp_at(step, other=0):
    f = lax.axis_index("fsdp")
    core = f % 2
    return lax.rem(f // 2 + step, 4) * 2 + (1 - core if other else core)


def greet(devices):
    barrier = pltpu.get_barrier_semaphore()
    for d in devices:
        pl.semaphore_signal(barrier, inc=1, device_id=d, device_id_type=MESH)
    pl.semaphore_wait(barrier, len(devices))


class Ring:
    def __init__(self, pos, dev, own, place, chunks, send_sem, recv_sem, partner=None):
        self.pos, self.dev, self.own, self.place, self.chunks = pos, dev, own, place, chunks
        self.send_sem, self.recv_sem, self.partner = send_sem, recv_sem, partner
        self.right, self.left, self.far = [lax.rem(pos + s, 4) for s in (1, 3, 2)]

    def copy(self, kind, k, src, dst, device):
        return remote(src, dst, self.send_sem.at[kind, k], self.recv_sem.at[kind, k], device)

    def own_copies(self, k):
        mine = self.place(self.pos, k)
        out = [self.copy(0, k, self.own(k), mine, self.dev(self.right)), self.copy(1, k, self.own(k), mine, self.dev(self.left))]
        if self.partner is not None:
            out.append(self.copy(3, k, self.own(k), mine, self.partner))
        return out

    def onward(self, k, odd):
        source, target = (self.right, self.left) if odd else (self.left, self.right)
        ref = self.place(source, k)
        return self.copy(2, k, ref, ref, self.dev(target))

    def across(self, kind, k):
        ref = self.place({4: self.left, 5: self.right, 6: self.far}[kind], k)
        return self.copy(kind, k, ref, ref, self.partner)

    def arrived(self, kind, k, pos, *other):
        ref = self.place(pos, k, *other)
        self.copy(kind, k, ref, ref, self.dev(self.right)).wait_recv()

    def start(self, k):
        for c in self.own_copies(k):
            c.start()

    def relay(self, k, odd):
        for kind, pos, onward in ((0, self.left, not odd), (1, self.right, odd)):
            self.arrived(kind, k, pos)
            if onward:
                self.onward(k, odd).start()
            if self.partner is not None:
                self.across(4 + kind, k).start()

    def last(self, k):
        self.arrived(2, k, self.far)
        if self.partner is not None:
            self.across(6, k).start()

    def from_partner(self, k):
        for kind, pos in ((3, self.pos), (4, self.left), (5, self.right), (6, self.far)):
            self.arrived(kind, k, pos, 1)

    def drain(self):
        for k in range(self.chunks):
            for c in self.own_copies(k):
                c.wait_send()
            self.onward(k, k % 2 == 1).wait_send()
            if self.partner is not None:
                for kind in (4, 5, 6):
                    self.across(kind, k).wait_send()


def x_ring(own, place, send_sem, recv_sem):
    f = lax.axis_index("fsdp")
    core = f % 2

    def where(p, k, other=0):
        return place(p * 2 + (1 - core if other else core), k)

    return Ring(f // 2, lambda p: {"fsdp": p * 2 + core}, own, where, NB, send_sem, recv_sem, {"fsdp": fsdp_at(0, 1)})


X_SEMS = [DMA((7, NB)), DMA((7, NB))]
FIRST_SEMS = [DMA((2, 3, 2)), DMA((2, 3, 2))]
SECOND_SEMS = [DMA((2, 3, 4)), DMA((2, 3, 4))]


def x_neighbours():
    return [{"fsdp": fsdp_at(1)}, {"fsdp": fsdp_at(3)}, {"fsdp": fsdp_at(0, 1)}]


def yz():
    e = lax.axis_index("ep")
    z, y = e // 4, e % 4
    return z, y, (lambda p: {"ep": p * 4 + y}), (lambda p: {"ep": z * 4 + p})


def yz_neighbours():
    z, y, on_z, on_y = yz()
    return [f(lax.rem(p + s, 4)) for f, p in ((on_z, z), (on_y, y)) for s in (1, 3)]


def cut(ref, lanes, half, chunk=None):
    size = ref.shape[1 if lanes else 0] // 2
    span = pl.ds(half * size, size) if chunk is None else pl.ds(half * size + chunk * (size // 2), size // 2)
    return ref.at[:, span] if lanes else ref.at[span]


def first_rings(own, full, lanes, sems):
    z, y, on_z, on_y = yz()
    send, recv = sems
    return [
        Ring(y, on_y, lambda k: cut(own, lanes, 0, k), lambda p, k: cut(full.at[z * 4 + p], lanes, 0, k), 2, send.at[0], recv.at[0]),
        Ring(z, on_z, lambda k: cut(own, lanes, 1, k), lambda p, k: cut(full.at[p * 4 + y], lanes, 1, k), 2, send.at[1], recv.at[1]),
    ]


def second_rings(full, lanes, sems):
    z, y, on_z, on_y = yz()
    send, recv = sems
    by_z = lambda p, k: cut(full.at[p * 4 + k], lanes, 0)
    by_y = lambda p, k: cut(full.at[k * 4 + p], lanes, 1)
    return [
        Ring(z, on_z, lambda k: by_z(z, k), by_z, 4, send.at[0], recv.at[0]),
        Ring(y, on_y, lambda k: by_y(y, k), by_y, 4, send.at[1], recv.at[1]),
    ]


def start(rings):
    for k in range(rings[0].chunks):
        for r in rings:
            r.start(k)


def relay(rings, k):
    for r in rings:
        r.relay(k, k % 2 == 1)


def finish(rings):
    for r in rings:
        for k in range(r.chunks):
            r.last(k)
        r.drain()


def norm_block(view, nw_ref, stage, h_stage, h_out, sems, tok_major):
    load = pltpu.make_async_copy(view, stage, sems.at[0])
    load.start()
    load.wait()
    for tb in range(2):
        def rows(c, tb=tb):
            return (stage[tb, c] if tok_major else stage[c, tb]).astype(F32)

        def ssq_body(c, acc):
            xf = rows(c)
            return acc + jnp.sum(xf * xf, axis=0, keepdims=True)

        ssq = lax.fori_loop(0, NB, ssq_body, jnp.zeros((1, TB), F32))
        rstd = lax.rsqrt(ssq * (1.0 / D) + NORM_EPS)

        def h_body(c, carry, tb=tb, rstd=rstd):
            nw = nw_ref[c]
            nw2 = jnp.concatenate([nw, nw], axis=1)
            h_stage[pl.ds(pl.multiple_of(c * DS, DS), DS), tb * TB:(tb + 1) * TB] = (rows(c) * rstd * nw2).astype(BF)
            return carry

        lax.fori_loop(0, NB, h_body, 0)
    store = pltpu.make_async_copy(h_stage, h_out, sems.at[1])
    store.start()
    store.wait()


def first_kernel(
    x_ref, nw_ref, w_ref, idx_ref, wd_ref, x_all, h_all, w_all, idx_all, wd_all, wd_next,
    stage, h_stage, wd_in, wd_out, local_sem, norm_sem, small_send, small_recv, *sems,
):
    f, e = lax.axis_index("fsdp"), lax.axis_index("ep")
    greet([{"fsdp": fsdp_at(s, o)} for s, o in PEERS] + yz_neighbours())
    ring = x_ring(lambda k: x_ref.at[k], lambda owner, k: x_all.at[owner, k], *sems[:2])
    w_first = first_rings(w_ref, w_all, True, sems[2:4])
    w_second = second_rings(w_all, True, sems[4:6])
    d_first = first_rings(wd_out.at[0], wd_all, False, sems[6:])
    own = [pltpu.make_async_copy(src, dst, local_sem.at[i])
           for i, (src, dst) in enumerate((
               (w_ref, w_all.at[e]), (x_ref, x_all.at[f]), (wd_ref.at[:, f], wd_in.at[:, f]), (idx_ref, idx_all.at[f])))]
    after = [pltpu.make_async_copy(wd_out.at[0], wd_all.at[e], local_sem.at[4]), pltpu.make_async_copy(wd_out.at[1], wd_next, local_sem.at[5])]
    small = []
    for p, (s, o) in enumerate(PEERS):
        peer = fsdp_at(s, o)
        small.append(remote(wd_ref.at[:, peer], wd_in.at[:, f], small_send.at[0, p], small_recv.at[0, p], {"fsdp": peer}))
        small.append(remote(idx_ref, idx_all.at[f], small_send.at[1, p], small_recv.at[1, p], {"fsdp": peer}))
    start(w_first)
    for c in small + own:
        c.start()
    for k in range(NB):
        ring.start(k)
    for p, (s, o) in enumerate(PEERS):
        source = fsdp_at((4 - s) % 4, o)
        remote(wd_ref.at[:, 0], wd_in.at[:, source], small_send.at[0, p], small_recv.at[0, p], {"fsdp": source}).wait_recv()
        remote(idx_ref, idx_all.at[source], small_send.at[1, p], small_recv.at[1, p], {"fsdp": source}).wait_recv()
    for c in own[2:]:
        c.wait()
    for l in range(2):
        wd_out[l, :, :NB * FP] = jnp.swapaxes(wd_in[l].reshape(NB * FP, DS), 0, 1)
        wd_out[l, :, NB * FP:] = jnp.zeros((DS, KP - NB * FP), BF)
    relay(w_first, 0)
    for k in range(NB):
        ring.relay(k, k % 2 == 1)
        if k == 0:
            relay(w_first, 1)
            for c in after:
                c.start()
            start(d_first)
        if k == 3:
            finish(w_first)
            own[0].wait()
            start(w_second)
        if k in (5, 6):
            relay(d_first, k - 5)
    for k in range(NB):
        ring.last(k)
        if k in (0, 4):
            relay(w_second, k // 4)
    for k in range(NB):
        ring.from_partner(k)
    own[1].wait()
    for i in range(STEPS):
        if i < 2:
            relay(w_second, i + 2)
        norm_block(x_all.at[pl.ds(2 * i, 2)], nw_ref, stage, h_stage, h_all.at[i], norm_sem, True)
    finish(d_first)
    for c in after:
        c.wait()
    finish(w_second)
    ring.drain()
    for c in small:
        c.wait_send()


def first_exchange(xt, nw, w, idx, wd):
    return pl.pallas_call(
        first_kernel,
        out_shape=(
            shape((NB, NB, DS, TB)), shape((STEPS, D, TB2)), shape((E,) + w.shape), shape((NB,) + idx.shape, jnp.int32),
            shape((E, DS, KP)), shape((DS, KP))),
        in_specs=[IN_VMEM] * 5,
        out_specs=[ANY] * 6,
        scratch_shapes=[
            pltpu.VMEM((2, NB, DS, TB), BF), pltpu.VMEM((D, TB2), BF), pltpu.VMEM((2, NB, FP, DS), BF), pltpu.VMEM((2, DS, KP), BF),
            DMA((6,)), DMA((2,)), DMA((2, 7)), DMA((2, 7)),
        ] + X_SEMS + FIRST_SEMS + SECOND_SEMS + FIRST_SEMS,
        compiler_params=params(1),
        cost_estimate=cost(120),
        name="first_exchange",
    )(xt, nw, w, idx, wd)


def weight_loads(g, w_refs, rt_hbm, wv, w_sem, rt_sem):
    out = [pltpu.make_async_copy(rt_hbm, wv.at[g, pl.ds(GROWS, E)], rt_sem.at[g])]
    for i in range(GE):
        at = 0
        for n, w in enumerate(w_refs):
            size = w.shape[1]
            out.append(pltpu.make_async_copy(w.at[g * GE + i], wv.at[g, pl.ds(i * RE + at, size)], w_sem.at[g, n, i]))
            at += size
    return out


def up_block(h_ref, idx, wv, slots, logits, split, hook):
    slots[...] = jnp.zeros_like(slots)

    def group(g, carry):
        hook(g)
        res = jnp.dot(wv[g], h_ref[0], preferred_element_type=F32)
        logits[...] = res[GROWS:]
        for i in range(GE):
            at, parts = i * RE, []
            for n in (FA, FP - FA) if split else (FP,):
                parts.append(jax.nn.silu(res[at:at + n]) * res[at + n:at + 2 * n])
                at += 2 * n
            act = jnp.concatenate(parts, axis=0) if split else parts[0]
            for j in range(K):
                slots[j] = jnp.where(idx[j:j + 1] == g * GE + i, act, slots[j])
        return carry

    lax.fori_loop(0, STEPS, group, 0)
    eids = lax.broadcasted_iota(jnp.int32, (E, TB2), 0)
    chosen = idx[0:1] == eids
    for j in range(1, K):
        chosen = jnp.logical_or(chosen, idx[j:j + 1] == eids)
    lg = jnp.where(chosen, logits[...], -jnp.inf)
    ex = jnp.where(chosen, jnp.exp(lg - jnp.max(lg, axis=0, keepdims=True)), 0.0)
    return ex / jnp.sum(ex, axis=0, keepdims=True)


def both(ref):
    return jnp.concatenate([ref[0], ref[1]], axis=1)


def when_all(*conditions):
    out = conditions[0]
    for c in conditions[1:]:
        out = jnp.logical_and(out, c)
    return pl.when(out)


def up_hook(step, g, loads, ring, second):
    @pl.when(step == 0)
    def _():
        for c in loads(g):
            c.wait()

    @when_all(step >= 1, g == 3)
    def _():
        for tb in range(2):
            ring.relay(2 * step - 2 + tb, tb == 1)

    for k in range(4):
        @pl.when(step * STEPS + g == 4 + 3 * k)
        def _(k=k):
            relay(second, k)


def up_kernel(h_ref, idx_ref, rt_hbm, wd_part, w_a, w_b, a_all, g_ref, wd_all, wv, slots, logits, a_buf, w_sem, rt_sem, local_sem, *sems):
    step = pl.program_id(0)
    f = lax.axis_index("fsdp")
    mine = lambda owner: pl.ds(pl.multiple_of(owner * FP, 8), FP)
    ring = x_ring(lambda k: a_buf.at[k], lambda owner, k: a_all.at[k, :, mine(owner)], *sems[:2])
    second = second_rings(wd_all, False, sems[2:])
    loads = lambda g: weight_loads(g, (w_a, w_b), rt_hbm, wv, w_sem, rt_sem)

    def own_a(k):
        return pltpu.make_async_copy(a_buf.at[k], a_all.at[k, :, mine(f)], local_sem.at[k])

    @pl.when(step == 0)
    def _():
        for g in range(STEPS):
            for c in loads(g):
                c.start()
        greet(x_neighbours() + yz_neighbours())
        start(second)

    hook = lambda g: up_hook(step, g, loads, ring, second)
    gates = up_block(h_ref, both(idx_ref), wv, slots, logits, True, hook)
    for tb in range(2):
        a_buf[2 * step + tb] = slots[:, :, tb * TB:(tb + 1) * TB].astype(BF)
        g_ref[tb] = gates[:, tb * TB:(tb + 1) * TB]
    for tb in range(2):
        ring.start(2 * step + tb)
        own_a(2 * step + tb).start()

    @pl.when(step == 3)
    def _():
        for k in LATE:
            ring.relay(k, k % 2 == 1)
        for k in range(NB):
            ring.last(k)
        for k in range(NB):
            ring.from_partner(k)
            own_a(k).wait()
        ring.drain()
        finish(second)


def pair(*tail):
    return pl.BlockSpec((2,) + tail, lambda i: (i,) + (0,) * len(tail))


def routing(layer):
    return pl.BlockSpec((NB if layer else 2, None, K, TB), lambda i: (0 if layer else i, layer, 0, 0))


def whole(*dims):
    return pl.BlockSpec(dims, lambda i: (0,) * len(dims))


UP_SCRATCH = [
    pltpu.VMEM((STEPS, GROWS + E, D), BF),
    pltpu.VMEM((K, FP, TB2), F32),
    pltpu.VMEM((E, TB2), F32),
    pltpu.VMEM((NB, K, FP, TB), BF),
    DMA((STEPS, 2, GE)), DMA((STEPS,)), DMA((NB,)),
]


def up_proj(h, idx, rt, wd_part, w_a, w_b):
    return pl.pallas_call(
        up_kernel,
        grid=(STEPS,),
        out_shape=(shape((NB, K, NB * FP, TB)), shape((NB, E, TB), F32), shape((E, DS, KP))),
        in_specs=[pl.BlockSpec((1, D, TB2), lambda i: (i, 0, 0)), routing(0)] + [ANY] * 4,
        out_specs=(ANY, pair(E, TB), ANY),
        scratch_shapes=UP_SCRATCH + X_SEMS + SECOND_SEMS,
        input_output_aliases={3: 2},
        compiler_params=params(2),
        cost_estimate=cost(70),
        name="up_proj",
    )(h, idx, rt, wd_part, w_a, w_b)


def down_block(a_ref, idx_ref, g_ref, wd_ref, acc, hook):
    idx = both(idx_ref).astype(F32).astype(BF)
    acc[...] = jnp.zeros_like(acc)

    def group(g, carry):
        hook(g)
        for i in range(GE):
            e = g * GE + i
            ef = e.astype(F32).astype(BF)
            parts = []
            for tb in range(2):
                sel = jnp.zeros((NB * FP, TB), BF)
                for j in range(K):
                    row = idx[j:j + 1, tb * TB:(tb + 1) * TB]
                    sel = jnp.where(row == ef, a_ref[tb, j], sel)
                parts.append(sel)
            out = jnp.dot(wd_ref[e, :, :NB * FP], jnp.concatenate(parts, axis=1), preferred_element_type=F32)
            gate = jnp.concatenate([g_ref[0, pl.ds(e, 1)], g_ref[1, pl.ds(e, 1)]], axis=1)
            acc[...] += gate * out
        return carry

    lax.fori_loop(0, STEPS, group, 0)


def new_x(x, acc, tb):
    return (x.astype(F32) + acc[:, tb * TB:(tb + 1) * TB]).astype(BF)


def down_mid_kernel(
    a_ref, idx_ref, g_ref, x_ref, wd_hbm, nw_ref, wd_next, x_all, h_all, wd_all,
    acc, o_buf, stage, h_stage, wd_v, wd_sem, local_sem, norm_sem, *sems,
):
    step = pl.program_id(0)
    f = lax.axis_index("fsdp")
    ring = x_ring(lambda k: o_buf.at[k], lambda owner, k: x_all.at[owner, k], *sems[:2])
    d_first = first_rings(wd_next, wd_all, False, sems[2:])
    own_wd = pltpu.make_async_copy(wd_next, wd_all.at[lax.axis_index("ep")], local_sem.at[NB])

    def own_x(k):
        return pltpu.make_async_copy(o_buf.at[k], x_all.at[f, k], local_sem.at[k])

    def wd_load(g):
        return pltpu.make_async_copy(wd_hbm.at[pl.ds(g * GE, GE)], wd_v.at[pl.ds(g * GE, GE)], wd_sem.at[g])

    @pl.when(step == 0)
    def _():
        for g in range(STEPS):
            wd_load(g).start()
        greet(x_neighbours() + yz_neighbours())
        own_wd.start()
        start(d_first)

    def hook(g):
        @pl.when(step == 0)
        def _():
            wd_load(g).wait()

        @pl.when(jnp.logical_and(step >= 2, g == 2))
        def _():
            for tb in range(2):
                ring.relay(2 * step - 4 + tb, tb == 1)
            for k in range(2):
                @pl.when(step == 2 + k)
                def _(k=k):
                    relay(d_first, k)

    down_block(a_ref, idx_ref, g_ref, wd_v, acc, hook)
    for tb in range(2):
        o_buf[2 * step + tb] = new_x(x_ref[tb, 0], acc, tb)
    for tb in range(2):
        ring.start(2 * step + tb)
        own_x(2 * step + tb).start()

    @pl.when(step == 3)
    def _():
        for i in range(STEPS):
            for k in (2 * i, 2 * i + 1):
                ring.last(k)
            for k in (2 * i, 2 * i + 1):
                ring.from_partner(k)
                own_x(k).wait()
            norm_block(x_all.at[:, pl.ds(2 * i, 2)], nw_ref, stage, h_stage, h_all.at[i], norm_sem, False)
            if i < 2:
                for k in (2 * i + 4, 2 * i + 5):
                    ring.relay(k, k % 2 == 1)
        ring.drain()
        own_wd.wait()
        finish(d_first)


def down_mid(a, idx, gates, x_all, wd, nw, wd_next):
    return pl.pallas_call(
        down_mid_kernel,
        grid=(STEPS,),
        out_shape=(shape((NB, NB, DS, TB)), shape((STEPS, D, TB2)), shape((E, DS, KP))),
        in_specs=[
            pair(K, NB * FP, TB), routing(0), pair(E, TB),
            pl.BlockSpec((2, 1, DS, TB), lambda i: (i, lax.axis_index("fsdp"), 0, 0)),
            ANY, whole(NB, DS, 128), whole(DS, KP),
        ],
        out_specs=[ANY] * 3,
        scratch_shapes=[
            pltpu.VMEM((DS, TB2), F32), pltpu.VMEM((NB, DS, TB), BF), pltpu.VMEM((NB, 2, DS, TB), BF), pltpu.VMEM((D, TB2), BF),
            pltpu.VMEM((E, DS, KP), BF), DMA((STEPS,)), DMA((NB + 1,)), DMA((2,)),
        ] + X_SEMS + FIRST_SEMS,
        compiler_params=params(4),
        cost_estimate=cost(80),
        name="down_mid",
    )(a, idx, gates, x_all, wd, nw, wd_next)


CODES = (17, 74, 191, 228)


def turn(n):
    ring = lax.axis_index("fsdp") // 2
    place = (1 + 3 * (ring % 2)) * (1 + 15 * (ring // 2))
    out = 0
    for i in range(STEPS):
        out = out + jnp.where(n == i, (CODES[i] // place) % 4, 0)
    return out


def last_kernel(
    h_ref, idx_ref, rt_hbm, wd_part, w, x_ref, o_all, a_all, wd_all, wv, slots, logits, a_buf, w_sem, rt_sem, local_sem,
    g_v, wd_v, a_v, acc, o_buf, passing, wd_sem, a_sem, out_send, out_recv, pass_send, pass_recv, *sems,
):
    step = pl.program_id(0)
    f = lax.axis_index("fsdp")
    core = f % 2
    mine = lambda owner: pl.ds(pl.multiple_of(owner * FP, 8), FP)
    ring = x_ring(lambda k: a_buf.at[k], lambda owner, k: a_all.at[k, :, mine(owner)], *sems[:2])
    second = second_rings(wd_all, False, sems[2:])
    loads = lambda g: weight_loads(g, (w,), rt_hbm, wv, w_sem, rt_sem)

    def own_a(k):
        return pltpu.make_async_copy(a_buf.at[k], a_all.at[k, :, mine(f)], local_sem.at[k])

    def wd_load(g):
        return pltpu.make_async_copy(wd_all.at[pl.ds(g * GE, GE)], wd_v.at[pl.ds(g * GE, GE)], wd_sem.at[g])

    def a_load(n):
        return pltpu.make_async_copy(a_all.at[pl.ds(2 * turn(n), 2)], a_v.at[n % 2], a_sem.at[n % 2])

    def complete(chunks):
        for k in chunks:
            ring.from_partner(k)
            own_a(k).wait()

    @pl.when(step == 0)
    def _():
        for g in range(STEPS):
            for c in loads(g):
                c.start()
        greet([{"fsdp": fsdp_at(s, o)} for s, o in PEERS] + yz_neighbours())
        start(second)

    def hook(g):
        up_hook(step, g, loads, ring, second)

        @when_all(step == 3, g == 1)
        def _():
            for k in range(4):
                ring.last(k)

        @when_all(step == 3, g == 2)
        def _():
            complete(range(4))
            a_load(0).start()

    @pl.when(step < STEPS)
    def _():
        gates = up_block(h_ref, both(idx_ref.at[pl.ds(2 * step, 2)]), wv, slots, logits, False, hook)
        for tb in range(2):
            a_buf[2 * step + tb] = slots[:, :, tb * TB:(tb + 1) * TB].astype(BF)
            g_v[2 * step + tb] = gates[:, tb * TB:(tb + 1) * TB]
        for tb in range(2):
            ring.start(2 * step + tb)
            own_a(2 * step + tb).start()

    n = step - STEPS

    @pl.when(n == 0)
    def _():
        finish(second)
        for g in range(STEPS):
            wd_load(g).start()

    def down_hook(g):
        @pl.when(n == 0)
        def _():
            wd_load(g).wait()

        @when_all(n == 0, g == 1)
        def _():
            for k in MIDDLE:
                ring.last(k)

        @when_all(n == 0, g == 2)
        def _():
            complete(MIDDLE)
            a_load(1).start()

        @when_all(n == 1, g == 0)
        def _():
            for k in LATE:
                ring.relay(k, k % 2 == 1)

        @when_all(n == 1, g == 3)
        def _():
            for k in LATE:
                ring.last(k)

        @when_all(n == 2, g == 0)
        def _():
            a_load(3).start()

        @when_all(n == 3, g == 3)
        def _():
            for other in range(2):
                send_by(0, other).wait_recv()
                passed(other).start()

    def send(i, other):
        part = 1 - core if other else core
        return remote(o_buf.at[i, part], o_all.at[f], out_send.at[i, other], out_recv.at[f], {"fsdp": 2 * turn(i) + part})

    def send_by(i, other):
        near = {"fsdp": fsdp_at(3 if other else 1)}
        return remote(o_buf.at[i, 1 - core if other else core], passing.at[other], out_send.at[i, other], pass_recv.at[other], near)

    def passed(other):
        source = fsdp_at(1 if other else 3)
        return remote(
            passing.at[other], o_all.at[source], pass_send.at[other], out_recv.at[source], {"fsdp": fsdp_at(3 if other else 1, other)})

    @pl.when(n >= 0)
    def _():
        now = 2 * turn(n)
        a_load(n).wait()
        down_block(a_v.at[n % 2], idx_ref.at[pl.ds(now, 2)], g_v.at[pl.ds(now, 2)], wd_v, acc, down_hook)
        for tb in range(2):
            o_buf[n, tb] = new_x(x_ref[0, now + tb], acc, tb)
        away = lax.rem(turn(n) + 4 - f // 2, 4)

        @pl.when(away == 2)
        def _():
            for other in range(2):
                send_by(n, other).start()

        @pl.when(away != 2)
        def _():
            send(n, 1).start()

        @pl.when(away % 2 == 1)
        def _():
            send(n, 0).start()

        @pl.when(n == 1)
        def _():
            complete(LATE)
            a_load(2).start()

    @pl.when(n == 3)
    def _():
        own = pltpu.make_async_copy(o_buf.at[3, core], o_all.at[f], a_sem.at[0])
        own.start()
        ring.drain()
        for s, o in PEERS:
            source = fsdp_at(s, o)
            remote(o_buf.at[0, 0], o_all.at[source], out_send.at[0, 0], out_recv.at[source], {"fsdp": source}).wait_recv()
        for i in range(STEPS):
            send_by(i, 1).wait_send()
            if i < 3:
                send_by(i, 0).wait_send()
        for other in range(2):
            passed(other).wait_send()
        own.wait()


def last_layer(h, idx, rt, wd_part, w, x_all):
    return pl.pallas_call(
        last_kernel,
        grid=(2 * STEPS,),
        out_shape=(shape((NB, DS, TB)), shape((NB, K, NB * FP, TB)), shape((E, DS, KP))),
        in_specs=[
            pl.BlockSpec((1, D, TB2), lambda i: (jnp.minimum(i, STEPS - 1), 0, 0)), routing(1), ANY, ANY, ANY,
            pl.BlockSpec((1, NB, DS, TB), lambda i: (lax.axis_index("fsdp"), 0, 0, 0), pipeline_mode=pl.Buffered(1)),
        ],
        out_specs=[ANY] * 3,
        scratch_shapes=UP_SCRATCH + [
            pltpu.VMEM((NB, E, TB), F32), pltpu.VMEM((E, DS, KP), BF), pltpu.VMEM((2, 2, K, NB * FP, TB), BF),
            pltpu.VMEM((DS, TB2), F32), pltpu.VMEM((STEPS, 2, DS, TB), BF),
            pltpu.VMEM((2, DS, TB), BF), DMA((STEPS,)), DMA((2,)), DMA((4, 2)), DMA((NB,)), DMA((2,)), DMA((2,)),
        ] + X_SEMS + SECOND_SEMS,
        input_output_aliases={3: 2},
        compiler_params=params(3),
        cost_estimate=cost(110),
        name="last_layer",
    )(h, idx, rt, wd_part, w, x_all)


def solution(mesh):
    tok_spec = P(("rep", "ep", "fsdp"), None)
    idx_spec = P(None, ("rep", "ep", "fsdp"), None)
    in_specs = (tok_spec, P(None, None), P(None, None, None), P(None, "ep", None, "fsdp"), P(None, "ep", None, "fsdp"), P(None, "ep", "fsdp", None), idx_spec)

    def local_program(x, norm_w, router_w, w_gate, w_up, w_down, expert_idx):
        pad = jnp.zeros((FP - F, D), BF)
        nws = [jnp.broadcast_to(n.reshape(NB, DS, 1), (NB, DS, 128)) for n in norm_w]
        routers = [r.T for r in router_w]

        def pack(gate, up):
            gate, up = gate.T, up.T
            return [gate[:FA], up[:FA]], [gate[FA:], pad, up[FA:], pad]

        part_a, part_b = [jnp.concatenate(p, axis=0) for p in pack(w_gate[0, 0], w_up[0, 0])]
        w_a = lax.all_gather(part_a, "ep", axis=0, tiled=False)
        gate1, up1, _ = lax.optimization_barrier((w_gate, w_up, part_a))
        rows = jnp.concatenate([gate1[1, 0].T, pad, up1[1, 0].T, pad], axis=0)
        wd = jnp.pad(w_down[:, 0], ((0, 0), (0, FP - F), (0, 0))).reshape(2, FP, NB, DS).swapaxes(1, 2)
        xt = x.T.reshape(NB, DS, TB)
        xt, idx, wd, part_b, rows, nws, routers = lax.optimization_barrier((xt, jnp.swapaxes(expert_idx, 1, 2), wd, part_b, rows, nws, routers))
        x_all, h, w_b, idx, wd_part, wd_next = first_exchange(xt, nws[0], part_b, idx, wd)
        rows, _ = lax.optimization_barrier((rows, idx))
        w_next = lax.all_gather(rows, "ep", axis=0, tiled=False)
        a, gates, wd_all = up_proj(h, idx, routers[0], wd_part, w_a, w_b)
        x_all, h, wd_part = down_mid(a, idx, gates, x_all, wd_all, nws[1], wd_next)
        return last_layer(h, idx, routers[1], wd_part, w_next, x_all)[0].reshape(D, TB).T

    return jax.shard_map(local_program, mesh=mesh, in_specs=in_specs, out_specs=tok_spec, check_vma=False)
```
